256 devices in a mesh: dp: 16 (over x, z_lo), ctx: 16 (over z_hi, y, core).
Axes of the slice: x: 4, y: 4, z: 8 (z_hi: 2, z_lo: 4; z = z_hi * 4 + z_lo), core: 2. Of those that a mesh axis runs over, the one named last changes fastest.
Arguments:
- stream: bfloat16 [16, 2048, 4096], P('dp', 'ctx'), may hold values from -6 to 6
- queries: bfloat16 [16, 2048, 2048], P('dp', 'ctx'), may hold values from -150 to 150
- keys: bfloat16 [16, 2048, 512], P('dp', 'ctx'), may hold values from -6 to 6
- values: bfloat16 [16, 2048, 512], P('dp', 'ctx'), may hold values from -6 to 6
- clip_lengths: int32 [16], P('dp'), may hold values from 1024 to 2048, as said below
- mod_shift: float32 [16, 4096], P('dp'), may hold values from -3 to 3
- mod_scale: float32 [16, 4096], P('dp'), may hold values from -0.5 to 0.5
- out_weight: bfloat16 [2048, 4096], P('ctx', 'dp'), may hold values from -4 to 4
- final_weight: bfloat16 [4096, 128], replicated, may hold values from -0.09375 to 0.09375
- noisy_latents: bfloat16 [16, 2048, 128], P('dp', 'ctx'), may hold values from -6 to 6
- timestep: int32 [16], P('dp'), may hold values from 100 to 599
- crop_map: int32 [16, 256], P('dp'), may hold values from 0 to 2047, as said below
- embed_weight: bfloat16 [128, 1408], replicated, may hold values from -0.5 to 0.5
- pre_gain: float32 [1408], replicated, may hold values from 0.1 to 1.9
- up_weight: bfloat16 [1408, 6144], P(None, 'ctx'), may hold values from -0.15625 to 0.15625
- down_weight: bfloat16 [6144, 1408], P('ctx'), may hold values from -0.21875 to 0.21875
- post_gain: float32 [1408], replicated, may hold values from 0.1 to 1.9
- head_weight: float32 [1408], replicated, may hold values from -4 to 4
Outputs:
- reward: float32 [16], P('dp')
- grad_stream: bfloat16 [16, 2048, 4096], P('dp', 'ctx')
- grad_queries: bfloat16 [16, 2048, 2048], P('dp', 'ctx')
The draws below stay inside these ranges and needn't reach their ends.
Inputs may be any that keep to these rules, and one draw needn't show every extreme that they name: `clip_lengths`: each clip's length lies between 1024 and 2048; in every draw some clip has length exactly 2048. `crop_map`: every crop token of clip b points below clip_lengths[b].
All inputs are finite; a program needn't handle non-finite values.
Results may differ from the reference program's by a relative error of at most 0.04.
Values may be sent and summed in bfloat16 or wider, within the bound.
No kernel may reach another device: no remote copies, remote signals or barrier semaphores. Data moves between devices by JAX's collectives and lax.ppermute only.
A program may use at most 128 MiB of HBM per device.

```python
import math
import jax
import jax.numpy as jnp
from jax import lax

D = 4096
HEADS = 16
KV_HEADS = 4
HEAD = 128
PATCH = 128
RW = 1408
RFF = 6144
S = 2048
BATCH = 16
ROWS = 256


def attention_fields(key):
    folded = jax.random.fold_in(key, 11)
    key_rows = jax.random.truncated_normal(jax.random.fold_in(folded, 1), -6.0, 6.0, (BATCH, S, KV_HEADS * HEAD), jnp.float32)
    query_rows = jax.random.truncated_normal(jax.random.fold_in(folded, 2), -6.0, 6.0, (BATCH, S, HEADS * HEAD), jnp.float32)
    return (query_rows, key_rows)


def draw_queries(key, part):
    return attention_fields(key)[0].astype(jnp.bfloat16)


def draw_keys(key, part):
    return attention_fields(key)[1].astype(jnp.bfloat16)


def length_draw(key):
    folded = jax.random.fold_in(key, 23)
    lengths = jax.random.randint(jax.random.fold_in(folded, 1), (BATCH,), S // 2, S + 1)
    longest = jax.random.randint(jax.random.fold_in(folded, 2), (), 0, BATCH)
    return jnp.where(jnp.arange(BATCH) == longest, S, lengths).astype(jnp.int32)


def draw_clip_lengths(key, part):
    return length_draw(key)


def draw_crop_map(key, part):
    lengths = length_draw(key)
    picks = jax.random.randint(jax.random.fold_in(key, 29), (BATCH, ROWS), 0, S)
    return (picks % lengths[:, None]).astype(jnp.int32)


def with_ends(drawn, key, low, top_value):
    index_at = [jax.random.randint(jax.random.fold_in(key, axis), (), 0, length) for axis, length in enumerate(drawn.shape)]
    widest = drawn.shape.index(max(drawn.shape))
    beside = index_at[:widest] + [(index_at[widest] + 1) % drawn.shape[widest]] + index_at[widest + 1:]
    return drawn.at[tuple(index_at)].set(low).at[tuple(beside)].set(top_value)


def with_spikes(drawn, key, source, target, parts, factor):
    def block_of(position):
        return (jnp.arange(drawn.shape[position]) // (drawn.shape[position] // parts)).reshape((-1,) + (1,) * (drawn.ndim - 1 - position))

    first = jax.random.permutation(key, parts)[block_of(target)]
    second = (block_of(target) + parts // 2) % parts
    return jnp.where((block_of(source) == first) | (block_of(source) == second), factor * drawn, drawn)


def levels(stream_key, dims, cuts, low, high):
    def one(position, blocks):
        steps = jax.random.uniform(jax.random.fold_in(jax.random.fold_in(stream_key, 6), position), (blocks,), jnp.float32, low / len(cuts), high / len(cuts))
        return jnp.repeat(jnp.exp(steps), dims[position] // blocks).reshape((-1,) + (1,) * (len(dims) - position - 1))

    gain = one(*cuts[0])
    for cut in cuts[1:]:
        gain = gain * one(*cut)
    return gain


def gaussian(key, shape, scale, limit, split=(), kind=jnp.bfloat16):
    gain = levels(key, shape, split, -0.22, 0.18) if split else 1.0
    entries = jax.random.normal(key, shape, jnp.float32) * scale * gain
    return jnp.minimum(jnp.maximum(entries, -limit), limit).astype(kind)


def bell_draw_with(stream_key, extent, deviation, bound, shards, heavy, kind=jnp.bfloat16):
    entries = deviation * jax.random.normal(stream_key, extent, jnp.float32)
    if shards:
        entries = entries * levels(stream_key, extent, shards, -0.22, 0.18)
    return jnp.clip(with_spikes(entries, jax.random.fold_in(stream_key, 3), *heavy), -bound, bound).astype(kind)


def setup_inputs(seed: int = 0) -> dict:
    key_of = jax.random.split(jax.random.key(seed), 19)
    stream = gaussian(key_of[0], (BATCH, S, D), 1.0, 6.0, ((0, 16), (1, 16)))
    queries = draw_queries(jax.random.fold_in(key_of[18], 71), 0)
    keys = draw_keys(jax.random.fold_in(key_of[18], 71), 0)
    values = gaussian(key_of[3], (BATCH, S, KV_HEADS * HEAD), 1.0, 6.0, ((0, 16), (1, 16)))
    clip_lengths = draw_clip_lengths(jax.random.fold_in(key_of[18], 71), 0)
    mod_shift = gaussian(key_of[5], (BATCH, D), 0.5, 3.0, ((0, 16),), jnp.float32)
    mod_scale = jnp.clip(jax.random.uniform(key_of[6], (BATCH, D), jnp.float32, -0.5, 0.5) * levels(key_of[6], (BATCH, D), ((0, 16),), -0.4, 0.0), -0.5, 0.5)
    out_weight = gaussian(key_of[7], (HEADS * HEAD, D), (max(1, 2 * HEADS * HEAD // S)) ** -0.5, 4.0, ((0, 16), (1, 16)))
    final_weight = gaussian(key_of[8], (D, PATCH), D ** -0.5, 0.09375)
    noisy_latents = gaussian(key_of[9], (BATCH, S, PATCH), 1.0, 6.0, ((0, 16), (1, 16)))
    timestep = with_ends(jax.random.randint(key_of[10], (BATCH,), 100, 600), jax.random.fold_in(key_of[10], 1), 100, 599).astype(jnp.int32)
    crop_map = draw_crop_map(jax.random.fold_in(key_of[18], 71), 0)
    embed_weight = gaussian(key_of[12], (PATCH, RW), PATCH ** -0.5, 0.5)
    pre_gain = jnp.clip(1.0 + 0.18 * jax.random.normal(key_of[13], (RW,), jnp.float32), 0.1, 1.9)
    up_weight = gaussian(key_of[14], (RW, RFF), RW ** -0.5, 0.15625, ((1, 16),))
    down_weight = bell_draw_with(key_of[15], (RFF, RW), (RFF // 4) ** -0.5, 0.21875, ((0, 16),), (0, 1, 16, 2.0))
    post_gain = jnp.clip(1.0 + 0.18 * jax.random.normal(key_of[16], (RW,), jnp.float32), 0.1, 1.9)
    head_weight = gaussian(key_of[17], (RW,), 1.0, 4.0, (), jnp.float32)
    return dict(stream=stream, queries=queries, keys=keys, values=values, clip_lengths=clip_lengths, mod_shift=mod_shift, mod_scale=mod_scale, out_weight=out_weight, final_weight=final_weight, noisy_latents=noisy_latents, timestep=timestep, crop_map=crop_map, embed_weight=embed_weight, pre_gain=pre_gain, up_weight=up_weight, down_weight=down_weight, post_gain=post_gain, head_weight=head_weight)


MASKED = -1e+30
LOSS_SCALE = 16.0
EPSILON = 1e-06

def rounded(amount):
    return lax.optimization_barrier(amount.astype(jnp.bfloat16)).astype(jnp.float32)

def plan(noise_step):
    phase = (noise_step.astype(jnp.float32) / 1000.0 + 0.008) / 1.008 * (math.pi / 2.0)
    signal_root = jnp.cos(phase)
    return (signal_root, jnp.sqrt(1.0 - signal_root * signal_root))

def gelu_slope(hidden, upstream):
    return jax.vjp(lambda argument: jax.nn.gelu(argument, approximate=True), hidden)[1](upstream)[0]

def reward_model(crop_tokens, embed_weight, pre_gain, up_weight, down_weight, post_gain, head_weight):
    row_total = crop_tokens.shape[0]
    embedded = jnp.dot(crop_tokens, embed_weight, preferred_element_type=jnp.float32)
    first_root = jnp.sqrt(lax.optimization_barrier(jnp.mean(embedded * embedded, axis=-1, keepdims=True)) + EPSILON)
    first_unit = embedded / first_root
    normed = (first_unit * pre_gain).astype(jnp.bfloat16)
    hidden = jnp.dot(normed, up_weight, preferred_element_type=jnp.float32)
    active = jax.nn.gelu(hidden, approximate=True).astype(jnp.bfloat16)
    summed = embedded + jnp.dot(active, down_weight, preferred_element_type=jnp.float32)
    second_root = jnp.sqrt(lax.optimization_barrier(jnp.mean(summed * summed, axis=-1, keepdims=True)) + EPSILON)
    second_unit = summed / second_root
    reward = jnp.mean(lax.optimization_barrier(jnp.sum(second_unit * post_gain * head_weight, axis=-1)))
    head_slope = -(LOSS_SCALE / row_total) * head_weight * post_gain
    summed_slope = (head_slope - second_unit * lax.optimization_barrier(jnp.mean(head_slope * second_unit, axis=-1, keepdims=True))) / second_root
    active_slope = jnp.dot(summed_slope.astype(jnp.bfloat16), down_weight.T, preferred_element_type=jnp.float32)
    hidden_slope = gelu_slope(hidden, active_slope).astype(jnp.bfloat16)
    normed_slope = jnp.dot(hidden_slope, up_weight.T, preferred_element_type=jnp.float32) * pre_gain
    embed_slope = summed_slope + (normed_slope - first_unit * lax.optimization_barrier(jnp.mean(normed_slope * first_unit, axis=-1, keepdims=True))) / first_root
    token_slope = jnp.dot(embed_slope.astype(jnp.bfloat16), embed_weight.T, preferred_element_type=jnp.float32)
    return (reward, token_slope)

def clip_pass(operands, weights):
    stream, queries, keys, values, clip_length, mod_shift, mod_scale, noisy_rows, noise_step, crop_rows = operands
    out_weight, final_weight, embed_weight, pre_gain, up_weight, down_weight, post_gain, head_weight = weights
    sequence = queries.shape[0]
    per_group = HEADS // KV_HEADS
    is_live = jnp.arange(sequence, dtype=jnp.int32) < clip_length
    query_heads = jnp.transpose(queries.reshape(sequence, KV_HEADS, per_group, HEAD), (1, 0, 2, 3))
    key_heads = jnp.transpose(keys.reshape(sequence, KV_HEADS, HEAD), (1, 0, 2))
    value_heads = jnp.transpose(values.reshape(sequence, KV_HEADS, HEAD), (1, 0, 2))

    def scores_of(query_block, key_block):
        scores = jnp.einsum('tgd,sd->gts', query_block.astype(jnp.float32), key_block.astype(jnp.float32)) / math.sqrt(HEAD)
        return jnp.where(is_live[None, None, :], scores, MASKED)

    def attend(blocks):
        query_block, key_block, value_block = blocks
        scores = scores_of(query_block, key_block)
        highest = lax.optimization_barrier(jnp.max(scores, axis=-1, keepdims=True))
        weights_rows = jnp.exp(scores - highest)
        denominator = lax.optimization_barrier(jnp.sum(weights_rows, axis=-1, keepdims=True))
        blended = jnp.einsum('gts,sd->gtd', rounded(weights_rows), value_block.astype(jnp.float32)) / denominator
        return (blended, (highest + jnp.log(denominator))[..., 0])
    blended, log_total = lax.map(attend, (query_heads, key_heads, value_heads))
    attended = jnp.transpose(blended, (2, 0, 1, 3)).reshape(sequence, HEADS * HEAD).astype(jnp.bfloat16)
    residual = stream.astype(jnp.float32) + jnp.dot(attended, out_weight, preferred_element_type=jnp.float32)
    centred = residual - lax.optimization_barrier(jnp.mean(residual, axis=-1, keepdims=True))
    inverse = lax.rsqrt(lax.optimization_barrier(jnp.mean(centred * centred, axis=-1, keepdims=True)) + EPSILON)
    unit_rows = centred * inverse
    gain_rows = 1.0 + mod_scale
    modulated = (unit_rows * gain_rows + mod_shift).astype(jnp.bfloat16)
    predicted = jnp.dot(modulated, final_weight, preferred_element_type=jnp.float32)
    signal_root, noise_root = plan(noise_step)
    denoised = ((noisy_rows.astype(jnp.float32) - noise_root * predicted) / signal_root).astype(jnp.bfloat16)
    crop_tokens = denoised[crop_rows]
    reward, token_slope = reward_model(crop_tokens, embed_weight, pre_gain, up_weight, down_weight, post_gain, head_weight)
    latent_slope = jnp.zeros((sequence, PATCH), jnp.float32).at[crop_rows].add(token_slope)
    noise_slope = (-(noise_root / signal_root) * latent_slope).astype(jnp.bfloat16)
    modulated_slope = jnp.dot(noise_slope, final_weight.T, preferred_element_type=jnp.float32) * gain_rows
    residual_slope = (modulated_slope - lax.optimization_barrier(jnp.mean(modulated_slope, axis=-1, keepdims=True)) - unit_rows * lax.optimization_barrier(jnp.mean(modulated_slope * unit_rows, axis=-1, keepdims=True))) * inverse
    grad_stream = residual_slope.astype(jnp.bfloat16)
    attended_slope = jnp.dot(grad_stream, out_weight.T, preferred_element_type=jnp.float32).astype(jnp.bfloat16)
    slope_heads = jnp.transpose(attended_slope.reshape(sequence, KV_HEADS, per_group, HEAD), (1, 0, 2, 3))
    attended_heads = jnp.transpose(attended.reshape(sequence, KV_HEADS, per_group, HEAD), (1, 0, 2, 3))

    def query_grad(blocks):
        query_block, key_block, value_block, slope_block, attended_block, log_block = blocks
        scores = scores_of(query_block, key_block)
        weights_rows = jnp.exp(scores - log_block[..., None])
        row_delta = lax.optimization_barrier(jnp.sum(slope_block.astype(jnp.float32) * attended_block.astype(jnp.float32), axis=-1)).T
        slopes = jnp.einsum('tgd,sd->gts', slope_block.astype(jnp.float32), value_block.astype(jnp.float32))
        score_slope = rounded(weights_rows * (slopes - row_delta[..., None]))
        return jnp.einsum('gts,sd->gtd', score_slope, key_block.astype(jnp.float32)) / math.sqrt(HEAD)
    gradients = lax.map(query_grad, (query_heads, key_heads, value_heads, slope_heads, attended_heads, log_total))
    grad_queries = jnp.transpose(gradients, (2, 0, 1, 3)).reshape(sequence, HEADS * HEAD).astype(jnp.bfloat16)
    return (reward, grad_stream, grad_queries)

def reference(stream, queries, keys, values, clip_lengths, mod_shift, mod_scale, out_weight, final_weight, noisy_latents, timestep, crop_map, embed_weight, pre_gain, up_weight, down_weight, post_gain, head_weight):
    weights = (out_weight, final_weight, embed_weight, pre_gain, up_weight, down_weight, post_gain, head_weight)
    reward, grad_stream, grad_queries = lax.map(lambda operands: clip_pass(operands, weights), (stream, queries, keys, values, clip_lengths, mod_shift, mod_scale, noisy_latents, timestep, crop_map))
    return (reward, grad_stream, grad_queries)
```

```python
import math

import jax
import jax.numpy as jnp
from jax import lax
from jax.sharding import Mesh, PartitionSpec as P

HEADS = 16
KV_HEADS = 4
HEAD = 128
PATCH = 128
CHIPS = 8

MASKED = -1e30
LOSS_SCALE = 16.0
EPSILON = 1e-06

F32 = jnp.float32
BF16 = jnp.bfloat16
CHIP = ("zh", "y")


def dot(a, b, dims):
    return lax.dot_general(a, b, (dims, ((), ())), preferred_element_type=F32)


def mm(a, b):
    return dot(a, b, ((1,), (0,)))


def mt(a, b):
    return dot(a, b, ((1,), (1,)))


def exchange(pieces, axis):
    return lax.all_to_all(pieces, axis, split_axis=0, concat_axis=0, tiled=True)


def copies(value, axis):
    size = lax.axis_size(axis)
    return exchange(jnp.broadcast_to(value, (size, *value.shape)), axis)


def swap(value, axis="core"):
    return lax.ppermute(value, axis, [(0, 1), (1, 0)])


def ring_blocks(value, axis):
    size = lax.axis_size(axis)
    blocks = [value]
    for step in range(1, size):
        blocks.append(lax.ppermute(value, axis, [((i + step) % size, i) for i in range(size)]))
    return blocks


def in_order(blocks, axis):
    size = len(blocks)
    if size == 1:
        return jnp.stack(blocks)
    twice = jnp.stack(blocks + blocks)
    start = lax.rem(size - lax.axis_index(axis), size)
    return lax.dynamic_slice_in_dim(twice, start, size, 0)


def plan(noise_step):
    phase = (noise_step.astype(F32) / 1000.0 + 0.008) / 1.008 * (math.pi / 2.0)
    signal_root = jnp.cos(phase)
    return (signal_root, jnp.sqrt(1.0 - signal_root * signal_root))


def gelu_slope(hidden, upstream):
    return jax.vjp(lambda argument: jax.nn.gelu(argument, approximate=True), hidden)[1](upstream)[0]


def split3(value):
    first = value.astype(BF16)
    rest = value - first.astype(F32)
    second = rest.astype(BF16)
    third = (rest - second.astype(F32)).astype(BF16)
    return first, second, third


def per_device(
    stream,
    queries,
    keys,
    values,
    clip_lengths,
    mod_shift,
    mod_scale,
    out_weight,
    final_weight,
    noisy_latents,
    timestep,
    crop_map,
    embed_weight,
    pre_gain,
    up_weight,
    down_weight,
    post_gain,
    head_weight,
):
    tokens = queries.shape[1]
    width = stream.shape[2]
    crop = crop_map[0]
    rows = crop.shape[0]
    half = rows // 2
    share = half // CHIPS
    core = lax.axis_index("core")
    zh = lax.axis_index("zh")
    y = lax.axis_index("y")
    chip = zh * 4 + y
    is_first = core == 0

    by_zl = in_order(ring_blocks(out_weight, "zl"), "zl")
    by_dp = in_order(ring_blocks(by_zl, "x"), "x")
    own_weight = jnp.transpose(by_dp.reshape(-1, *out_weight.shape), (1, 0, 2)).reshape(
        out_weight.shape[0], width
    )
    chip_weight = jnp.concatenate([own_weight, swap(own_weight)], axis=0)
    chip_stream = jnp.concatenate([stream[0], swap(stream[0])], axis=0)
    chip_noisy = jnp.concatenate([noisy_latents[0], swap(noisy_latents[0])], axis=0)
    up_pair = jnp.concatenate([up_weight, swap(up_weight)], axis=1)
    down_pair = jnp.concatenate([down_weight, swap(down_weight)], axis=0)

    query_pairs = queries[0].reshape(tokens, CHIPS, 2, HEAD)
    query_pairs = jnp.where(is_first, query_pairs, query_pairs[:, :, ::-1])
    query_pairs = jnp.transpose(query_pairs.reshape(tokens, CHIPS, 2 * HEAD), (1, 0, 2))

    def for_chips(side):
        heads = jnp.transpose(side.reshape(tokens, KV_HEADS, HEAD), (1, 0, 2))
        return jnp.repeat(heads, CHIPS // KV_HEADS, axis=0)

    sent = jnp.concatenate([query_pairs, for_chips(keys[0]), for_chips(values[0])], axis=2)
    mine = exchange(sent, CHIP).reshape(CHIPS * tokens, 4 * HEAD)
    other = swap(mine[:, HEAD:])
    query_side = jnp.concatenate([mine[:, :HEAD], other[:, :HEAD]], axis=0)
    key_side = jnp.concatenate([mine[:, 2 * HEAD : 3 * HEAD], other[:, HEAD : 2 * HEAD]], axis=0)
    value_side = jnp.concatenate([mine[:, 3 * HEAD :], other[:, 2 * HEAD :]], axis=0)

    place = jnp.arange(2 * CHIPS * tokens, dtype=jnp.int32)
    place_core = jnp.where(place < CHIPS * tokens, core, 1 - core)
    place_rest = place % (CHIPS * tokens)
    token_at = (place_rest // tokens) * (2 * tokens) + place_core * tokens + place_rest % tokens
    crop_core = (crop // tokens) % 2
    crop_at = (
        jnp.where(crop_core == core, 0, CHIPS * tokens)
        + (crop // (2 * tokens)) * tokens
        + crop % tokens
    )
    query_rows = jnp.take(query_side, crop_at, axis=0, mode="clip")

    scores = mt(query_rows, key_side) * (1.0 / math.sqrt(HEAD))
    scores = jnp.where(token_at < clip_lengths[0], scores, MASKED)
    highest = jnp.max(scores, axis=-1, keepdims=True)
    weights = jnp.exp(scores - highest)
    denominator = jnp.sum(weights, axis=-1, keepdims=True)
    weights = weights.astype(BF16)
    attended = (mm(weights, value_side) / denominator).astype(BF16)

    kept = lax.dynamic_slice_in_dim(attended, core * half, half, 0)
    given = lax.dynamic_slice_in_dim(attended, (1 - core) * half, half, 0)
    attended_pair = jnp.concatenate([kept, swap(given)], axis=1)
    crop_half = lax.dynamic_slice_in_dim(crop, core * half, half, 0)
    pair_place = jnp.arange(2 * tokens, dtype=jnp.int32)
    pair_token = chip * (2 * tokens) + jnp.where(
        pair_place < tokens, core * tokens + pair_place, (1 - core) * tokens + pair_place - tokens
    )
    pick = (crop_half[:, None] == pair_token[None, :]).astype(BF16)
    partial = mm(attended_pair, chip_weight) + mm(pick, chip_stream)
    partial = jnp.concatenate([partial, mm(pick, chip_noisy)], axis=1).astype(BF16)
    arrived = exchange(partial.reshape(CHIPS, share, width + PATCH), CHIP)
    arrived = arrived.astype(F32).sum(axis=0)
    residual = arrived[:, :width]
    noisy = arrived[:, width:]

    centred = residual - jnp.mean(residual, axis=-1, keepdims=True)
    inverse = lax.rsqrt(jnp.mean(centred * centred, axis=-1, keepdims=True) + EPSILON)
    unit_rows = centred * inverse
    gain_rows = 1.0 + mod_scale[0]
    modulated = (unit_rows * gain_rows + mod_shift[0]).astype(BF16)
    predicted = mm(modulated, final_weight)
    signal_root, noise_root = plan(timestep[0])
    denoised = ((noisy - noise_root * predicted) / signal_root).astype(BF16)
    crop_tokens = copies(denoised, CHIP).reshape(half, PATCH)

    inverse_parts = jnp.concatenate(
        list(split3(inverse)) + [jnp.zeros((share, 125), BF16)], axis=1
    )
    unit_own = jnp.concatenate([unit_rows.astype(BF16), inverse_parts], axis=1)
    unit_pair = jnp.concatenate([unit_own, swap(unit_own, "zh")], axis=0)
    unit_half = jnp.concatenate(ring_blocks(unit_pair, "y"), axis=0)
    unit_all = jnp.concatenate([unit_half, swap(unit_half)], axis=0)
    spot = jnp.arange(rows, dtype=jnp.int32)
    spot_rest = spot % half
    spot_y = (y + spot_rest // (2 * share)) % 4
    spot_zh = jnp.where((spot_rest // share) % 2 == 0, zh, 1 - zh)
    spot_row = (
        jnp.where(spot < half, core, 1 - core) * half
        + (spot_zh * 4 + spot_y) * share
        + spot_rest % share
    )

    embedded = mm(crop_tokens, embed_weight)
    first_root = jnp.sqrt(jnp.mean(embedded * embedded, axis=-1, keepdims=True) + EPSILON)
    first_unit = embedded / first_root
    normed = (first_unit * pre_gain).astype(BF16)
    hidden = mm(normed, up_pair)
    active = jax.nn.gelu(hidden, approximate=True).astype(BF16)
    head_slope = -(LOSS_SCALE / rows) * head_weight * post_gain
    added = exchange(mm(active, down_pair).astype(BF16).reshape(CHIPS, share, -1), CHIP)
    summed = lax.dynamic_slice_in_dim(embedded, chip * share, share, 0) + added.astype(F32).sum(
        axis=0
    )
    second_root = jnp.sqrt(jnp.mean(summed * summed, axis=-1, keepdims=True) + EPSILON)
    second_unit = summed / second_root
    reward_part = jnp.sum(second_unit * post_gain * head_weight) / rows
    summed_slope = (
        head_slope - second_unit * jnp.mean(head_slope * second_unit, axis=-1, keepdims=True)
    ) / second_root
    slope_half = copies(summed_slope.astype(BF16), CHIP).reshape(half, -1)
    active_slope = mt(slope_half, down_pair)
    hidden_slope32 = gelu_slope(hidden, active_slope)
    hidden_slope = hidden_slope32.astype(BF16)
    gained_embed = (embed_weight.astype(F32) * pre_gain).astype(BF16)
    hidden_embed = mm(gained_embed, up_pair).astype(BF16)
    along = jnp.sum(hidden_slope32 * hidden, axis=-1, keepdims=True) / embedded.shape[1]
    unit_embed = mt(first_unit.astype(BF16), embed_weight)
    part = (mt(hidden_slope, hidden_embed) - along * unit_embed) / first_root
    reward_lanes = jnp.concatenate(
        [jnp.broadcast_to(piece.reshape(1, 1), (16, PATCH)) for piece in split3(reward_part)], axis=0
    )
    parts = copies(jnp.concatenate([part.astype(BF16), reward_lanes], axis=0), CHIP)
    parts = parts.astype(F32).sum(axis=0)
    token_half = parts[:half] + mt(slope_half, embed_weight)
    reward_half = parts[half : half + 8] + parts[half + 16 : half + 24] + parts[half + 32 : half + 40]
    both = jnp.concatenate([token_half, reward_half], axis=0)
    back = swap(both)
    reward = (both + back)[half, 0]
    token_slope = jnp.concatenate(
        [
            jnp.where(is_first, token_half, back[:half]),
            jnp.where(is_first, back[:half], token_half),
        ],
        axis=0,
    )
    same = crop[:, None] == crop[None, :]
    latent_slope = mm(same.astype(BF16), token_slope.astype(BF16))
    noise_slope = (-(noise_root / signal_root) * latent_slope).astype(BF16)

    gained = final_weight.astype(F32) * gain_rows[:, None]
    gained16 = gained.astype(BF16)
    weight_latent = mm(own_weight, gained16)
    weight_sum = jnp.sum(own_weight.astype(F32), axis=1)
    units = unit_all[:, :width]
    by_spot = jnp.concatenate(
        [
            mt(units, own_weight),
            mm(units, gained16) / width,
            unit_all[:, width:].astype(F32),
        ],
        axis=1,
    )
    canon = jnp.take(by_spot, jnp.zeros((rows,), jnp.int32).at[spot_row].set(spot), axis=0, mode="clip")
    unit_weight = canon[:, :HEAD]
    unit_latent = canon[:, HEAD : HEAD + PATCH]
    row_inverse = jnp.sum(canon[:, HEAD + PATCH :], axis=-1, keepdims=True)
    noise32 = noise_slope.astype(F32)
    row_mean = jnp.sum(noise32 * jnp.mean(gained, axis=0), axis=-1, keepdims=True)
    row_along = jnp.sum(noise32 * unit_latent, axis=-1, keepdims=True)
    attended_slope = (
        (mt(noise_slope, weight_latent.astype(BF16)) - row_mean * weight_sum - row_along * unit_weight)
        * row_inverse
    ).astype(BF16)
    row_delta = jnp.sum(attended_slope.astype(F32) * attended.astype(F32), axis=-1, keepdims=True)
    slopes = mt(attended_slope, value_side)
    score_slope = (weights.astype(F32) * ((slopes - row_delta) / denominator)).astype(BF16)
    query_slope = (mm(score_slope, key_side) * (1.0 / math.sqrt(HEAD))).astype(BF16)

    earlier = same & (jnp.arange(rows)[None, :] < jnp.arange(rows)[:, None])
    first_seen = jnp.logical_not(jnp.any(earlier, axis=1))
    label = jnp.where(first_seen, crop, -1)
    query_other = swap(query_slope)
    query_pair = jnp.concatenate(
        [
            jnp.where(is_first, query_slope, query_other),
            jnp.where(is_first, query_other, query_slope),
        ],
        axis=1,
    )
    spread = (token_at[: CHIPS * tokens, None] == label[None, :]).astype(BF16)
    spread_rows = mm(spread, query_pair).astype(BF16)
    home = exchange(spread_rows.reshape(CHIPS, tokens, 2 * HEAD), CHIP)
    grad_queries = jnp.transpose(home, (1, 0, 2)).reshape(tokens, HEADS * HEAD)

    own_token = (chip * 2 + core) * tokens + jnp.arange(tokens, dtype=jnp.int32)
    spot_label = jnp.sum(
        jnp.where(spot_row[:, None] == jnp.arange(rows, dtype=jnp.int32)[None, :], label[None, :], 0),
        axis=1,
    )
    own_spots = (own_token[:, None] == spot_label[None, :]).astype(BF16)
    own_units = mm(own_spots, unit_all)
    own_inverse = jnp.sum(own_units[:, width:], axis=-1, keepdims=True)
    own_units = own_units[:, :width]
    own_rows = (own_token[:, None] == label[None, :]).astype(BF16)
    own_noise = mm(own_rows, noise_slope).astype(BF16)
    modulated_slope = mt(own_noise, final_weight) * gain_rows
    grad_stream = (
        (
            modulated_slope
            - jnp.mean(modulated_slope, axis=-1, keepdims=True)
            - own_units * jnp.mean(modulated_slope * own_units, axis=-1, keepdims=True)
        )
        * own_inverse
    ).astype(BF16)
    return (jnp.reshape(reward, (1,)), grad_stream[None], grad_queries[None])


DP = ("x", "zl")
CTX = ("zh", "y", "core")


def solution(mesh):
    across = mesh.shape["dp"]
    near = min(4, across)
    fine = Mesh(
        mesh.devices.reshape(across // near, near, 2, 4, 2), ("x", "zl", "zh", "y", "core")
    )
    return jax.shard_map(
        per_device,
        mesh=fine,
        in_specs=(
            P(DP, CTX, None),
            P(DP, CTX, None),
            P(DP, CTX, None),
            P(DP, CTX, None),
            P(DP),
            P(DP, None),
            P(DP, None),
            P(CTX, DP),
            P(),
            P(DP, CTX, None),
            P(DP),
            P(DP, None),
            P(),
            P(),
            P(None, CTX),
            P(CTX, None),
            P(),
            P(),
        ),
        out_specs=(P(DP), P(DP, CTX, None), P(DP, CTX, None)),
        check_vma=False,
    )
```

```python
import functools
import math

import jax
import jax.numpy as jnp
from jax import lax
from jax.experimental import pallas as pl
from jax.experimental.pallas import tpu as pltpu
from jax.sharding import Mesh, PartitionSpec as P


HEADS = 16
HEAD = 128
PATCH = 128
CHIPS = 8

MASKED = -1e30
LOSS_SCALE = 16.0
EPSILON = 1e-06

F32 = jnp.float32
BF16 = jnp.bfloat16
CHIP = ("zh", "y")
ROWS = ("y", "zh")
MIB = 1024 * 1024


def dot(a, b, dims):
    return lax.dot_general(a, b, (dims, ((), ())), preferred_element_type=F32)


def mm(a, b):
    return dot(a, b, ((1,), (0,)))


def mt(a, b):
    return dot(a, b, ((1,), (1,)))


def exchange(pieces, axis):
    return lax.all_to_all(pieces, axis, split_axis=0, concat_axis=0, tiled=True)


def swap(value, axis="core"):
    return lax.ppermute(value, axis, [(0, 1), (1, 0)])


def ring_blocks(value, axis):
    size = lax.axis_size(axis)
    blocks = [value]
    for step in range(1, size):
        blocks.append(lax.ppermute(value, axis, [((i + step) % size, i) for i in range(size)]))
    return blocks


def whole(shape):
    return pl.BlockSpec(shape, lambda _: (0,) * len(shape))


def kernel_call(body, outs, flops, moved, operands, scalars=None):
    specs = [whole(operand.shape) for operand in operands]
    if scalars is not None:
        specs = [pl.BlockSpec(memory_space=pltpu.SMEM)] + specs
        operands = [scalars] + operands
    return pl.pallas_call(
        body,
        grid=(1,),
        out_shape=[jax.ShapeDtypeStruct(shape, kind) for shape, kind in outs],
        in_specs=specs,
        out_specs=[whole(shape) for shape, _ in outs],
        cost_estimate=pl.CostEstimate(flops=flops, bytes_accessed=moved, transcendentals=0),
    )(*operands)


def pack_body(spots_ref, query_ref, key_ref, value_ref, out_ref):
    core = spots_ref[0]
    for chip in range(CHIPS):
        group = slice((chip // 2) * HEAD, (chip // 2 + 1) * HEAD)
        near = pl.multiple_of((2 * chip + core) * HEAD, HEAD)
        far = pl.multiple_of((2 * chip + 1 - core) * HEAD, HEAD)
        out_ref[chip, :, 0:HEAD] = query_ref[:, pl.ds(near, HEAD)]
        out_ref[chip, :, HEAD : 2 * HEAD] = query_ref[:, pl.ds(far, HEAD)]
        out_ref[chip, :, 2 * HEAD : 3 * HEAD] = key_ref[:, group]
        out_ref[chip, :, 3 * HEAD :] = value_ref[:, group]


def pick_rows(wanted, first, count):
    lanes = lax.broadcasted_iota(jnp.int32, (wanted.shape[0], count), 1) + first
    return (lanes == wanted).astype(F32).astype(BF16)


def attend_body(mine_ref, other_ref, at_ref, live_ref, att_ref, weights_ref, denominator_ref):
    span = mine_ref.shape[0]
    block = 128
    for start in range(0, at_ref.shape[0], block):
        here = slice(start, start + block)
        wanted = at_ref[here, :]
        query = mm(pick_rows(wanted, 0, span), mine_ref[:, 0:HEAD])
        query = query + mm(pick_rows(wanted, span, span), other_ref[:, HEAD : 2 * HEAD])
        query = query.astype(BF16)
        scale = 1.0 / math.sqrt(HEAD)
        first = mt(query, mine_ref[:, 2 * HEAD : 3 * HEAD]) * scale
        first = jnp.where(live_ref[:, 0:span] > 0, first, MASKED)
        second = mt(query, other_ref[:, 2 * HEAD : 3 * HEAD]) * scale
        second = jnp.where(live_ref[:, span:] > 0, second, MASKED)
        highest = jnp.maximum(
            jnp.max(first, axis=-1, keepdims=True), jnp.max(second, axis=-1, keepdims=True)
        )
        first = jnp.exp(first - highest)
        second = jnp.exp(second - highest)
        denominator = jnp.sum(first, axis=-1, keepdims=True) + jnp.sum(
            second, axis=-1, keepdims=True
        )
        first = first.astype(BF16)
        second = second.astype(BF16)
        blended = mm(first, mine_ref[:, 3 * HEAD :]) + mm(second, other_ref[:, 3 * HEAD :])
        att_ref[here, :] = (blended / denominator).astype(BF16)
        weights_ref[here, 0:span] = first
        weights_ref[here, span:] = second
        denominator_ref[here, :] = denominator


def project_body(near, across, index_ref, att_ref, att_other_ref, crop_ref, *refs):
    count = across
    own_refs, pair_refs, refs = refs[:count], refs[count : 2 * count], refs[2 * count :]
    stream_ref, stream_other_ref, noisy_ref, noisy_other_ref, out_ref, weight_ref = refs
    core, chip, x, zl = index_ref[0], index_ref[1], index_ref[2], index_ref[3]
    half = out_ref.shape[0]
    tokens = stream_ref.shape[0]
    width = stream_ref.shape[1]
    rows = pl.ds(pl.multiple_of(core * half, half), half)
    kept = att_ref[rows, :]
    other = att_other_ref[rows, :]
    wanted = crop_ref[rows, :] - chip * (2 * tokens)
    pick = pick_rows(wanted, core * tokens, tokens)
    pick_other = pick_rows(wanted, (1 - core) * tokens, tokens)
    for shift in range(across):
        for step in range(near):
            place = lax.rem(x + shift, across) * near + lax.rem(zl + step, near)
            size = own_refs[shift].shape[2]
            columns = pl.ds(pl.multiple_of(place * size, size), size)
            weight = own_refs[shift][step]
            weight_ref[:, columns] = weight
            total = mm(kept, weight) + mm(other, pair_refs[shift][step])
            total = total + mm(pick, stream_ref[:, columns])
            total = total + mm(pick_other, stream_other_ref[:, columns])
            out_ref[:, columns] = total.astype(BF16)
    noisy = mm(pick, noisy_ref[...]) + mm(pick_other, noisy_other_ref[...])
    out_ref[:, width:] = noisy.astype(BF16)


def slope_body(
    core_ref,
    factor_ref,
    token_ref,
    back_ref,
    crop_ref,
    crop_row_ref,
    weight_latent_ref,
    mean_ref,
    sum_ref,
    unit_weight_ref,
    unit_latent_ref,
    inverse_ref,
    att_ref,
    weights_ref,
    denominator_ref,
    mine_ref,
    other_ref,
    out_ref,
    noise_ref,
):
    span = mine_ref.shape[0]
    block = 128
    core = core_ref[0]
    half = out_ref.shape[0] // 2
    near, far = token_ref[0:half, :], back_ref[0:half, :]
    low = jnp.where(core == 0, near, far).astype(BF16)
    high = jnp.where(core == 0, far, near).astype(BF16)
    for start in range(0, out_ref.shape[0], block):
        here = slice(start, start + block)
        same = (crop_ref[here, :] == crop_row_ref[...]).astype(F32).astype(BF16)
        latent = mm(same[:, 0:half], low) + mm(same[:, half:], high)
        noise = (factor_ref[...] * latent).astype(BF16)
        noise_ref[here, :] = noise
        noise32 = noise.astype(F32)
        row_mean = jnp.sum(noise32 * mean_ref[...], axis=-1, keepdims=True)
        row_along = jnp.sum(noise32 * unit_latent_ref[here, :], axis=-1, keepdims=True)
        slope = mt(noise, weight_latent_ref[...]) - row_mean * sum_ref[...]
        slope = (slope - row_along * unit_weight_ref[here, :]) * inverse_ref[here, :]
        slope = slope.astype(BF16)
        delta = jnp.sum(slope.astype(F32) * att_ref[here, :].astype(F32), axis=-1, keepdims=True)
        recip = 1.0 / denominator_ref[here, :]
        first = mt(slope, mine_ref[:, 3 * HEAD :]) - delta
        first = (weights_ref[here, 0:span].astype(F32) * (first * recip)).astype(BF16)
        second = mt(slope, other_ref[:, 3 * HEAD :]) - delta
        second = (weights_ref[here, span:].astype(F32) * (second * recip)).astype(BF16)
        total = mm(first, mine_ref[:, 2 * HEAD : 3 * HEAD])
        total = total + mm(second, other_ref[:, 2 * HEAD : 3 * HEAD])
        out_ref[here, :] = (total * (1.0 / math.sqrt(HEAD))).astype(BF16)


def spread_body(core_ref, slope_ref, slope_other_ref, label_ref, out_ref):
    core = core_ref[0]
    tokens = out_ref.shape[1]
    own = slope_ref[...]
    other = slope_other_ref[...]
    left = jnp.where(core == 0, own, other)
    right = jnp.where(core == 0, other, own)
    for chip in range(CHIPS):
        token = lax.broadcasted_iota(jnp.int32, (tokens, 1), 0) + (2 * chip + core) * tokens
        pick = (token == label_ref[...]).astype(F32).astype(BF16)
        out_ref[chip, :, 0:HEAD] = mm(pick, left).astype(BF16)
        out_ref[chip, :, HEAD:] = mm(pick, right).astype(BF16)


def home_body(home_ref, out_ref):
    for chip in range(CHIPS):
        out_ref[:, chip * 2 * HEAD : (chip + 1) * 2 * HEAD] = home_ref[chip]


def partial_body(index_ref, arrived_ref, keep_ref, give_ref):
    zh = index_ref[1]
    share = keep_ref.shape[0]
    own = pl.ds(pl.multiple_of(zh * share, share), share)
    away = pl.ds(pl.multiple_of((1 - zh) * share, share), share)
    keep = arrived_ref[0, own, :].astype(F32)
    give = arrived_ref[0, away, :].astype(F32)
    for y in range(1, 4):
        keep = keep + arrived_ref[y, own, :].astype(F32)
        give = give + arrived_ref[y, away, :].astype(F32)
    keep_ref[...] = keep
    give_ref[...] = give.astype(BF16)


def split3(value):
    first = value.astype(BF16)
    rest = value - first.astype(F32)
    second = rest.astype(BF16)
    third = (rest - second.astype(F32)).astype(BF16)
    return first, second, third


def layer_body(
    keep_ref, got_ref, gain_ref, shift_ref, weight_ref, signal_ref, noise_ref, out_ref, unit_ref
):
    width = gain_ref.shape[1]
    residual = keep_ref[:, 0:width] + got_ref[:, 0:width].astype(F32)
    noisy = keep_ref[:, width:] + got_ref[:, width:].astype(F32)
    centred = residual - jnp.mean(residual, axis=-1, keepdims=True)
    inverse = lax.rsqrt(jnp.mean(centred * centred, axis=-1, keepdims=True) + EPSILON)
    unit = centred * inverse
    modulated = (unit * gain_ref[...] + shift_ref[...]).astype(BF16)
    predicted = mm(modulated, weight_ref[...])
    denoised = ((noisy - noise_ref[...] * predicted) / signal_ref[...]).astype(BF16)
    for chip in range(CHIPS):
        out_ref[chip] = denoised
    unit_ref[:, 0:width] = unit.astype(BF16)
    lane = lax.broadcasted_iota(jnp.int32, noisy.shape, 1)
    tail = jnp.zeros(noisy.shape, F32)
    for place, piece in enumerate(split3(inverse)):
        tail = jnp.where(lane == place, piece.astype(F32), tail)
    unit_ref[:, width:] = tail.astype(BF16)


def pair_body(index_ref, own_ref, got_ref, out_ref):
    zh = index_ref[1]
    share = own_ref.shape[0]
    out_ref[pl.ds(pl.multiple_of(zh * share, share), share), :] = own_ref[...]
    out_ref[pl.ds(pl.multiple_of((1 - zh) * share, share), share), :] = got_ref[...]


def half_body(index_ref, *refs):
    y = index_ref[2]
    out_ref = refs[-1]
    size = refs[0].shape[0]
    for shift, ref in enumerate(refs[:-1]):
        place = lax.rem(y + shift, 4)
        out_ref[pl.ds(pl.multiple_of(place * size, size), size), :] = ref[...]


def unit_body(index_ref, half_ref, other_ref, head_ref, latent_ref, weight_ref, along_ref, inverse_ref):
    core = index_ref[0]
    count = half_ref.shape[0]
    width = head_ref.shape[1]
    for ref, place in ((half_ref, core), (other_ref, 1 - core)):
        here = pl.ds(pl.multiple_of(place * count, count), count)
        weight_ref[here, :] = mt(ref[:, 0:width], head_ref[...])
        along_ref[here, :] = mm(ref[:, 0:width], latent_ref[...]) * (1.0 / width)
        inverse_ref[here, :] = jnp.sum(ref[:, width:].astype(F32), axis=-1, keepdims=True)


def norm_body(index_ref, embedded_ref, added_ref, gain_ref, head_ref, out_ref, reward_ref):
    share = added_ref.shape[1]
    rows = 2 * embedded_ref.shape[0]
    own = pl.ds(pl.multiple_of(index_ref[3] * share, share), share)
    summed = added_ref[0].astype(F32)
    for chip in range(1, CHIPS):
        summed = summed + added_ref[chip].astype(F32)
    summed = embedded_ref[own, :] + summed
    root = jnp.sqrt(jnp.mean(summed * summed, axis=-1, keepdims=True) + EPSILON)
    unit = summed / root
    gain, head = gain_ref[...], head_ref[...]
    head_slope = -(LOSS_SCALE / rows) * head * gain
    slope = (head_slope - unit * jnp.mean(head_slope * unit, axis=-1, keepdims=True)) / root
    slope = slope.astype(BF16)
    for chip in range(CHIPS):
        out_ref[chip] = slope
    reward = jnp.sum(unit * gain * head, axis=-1, keepdims=True)
    reward = jnp.sum(reward, axis=0, keepdims=True) / rows
    for place, piece in enumerate(split3(reward)):
        here = slice(place * 16, (place + 1) * 16)
        reward_ref[here, :] = jnp.broadcast_to(piece.astype(F32), (16, PATCH)).astype(BF16)


def back_body(
    slope_ref, down_ref, hidden_ref, latent_ref, embed_ref, root_ref, reward_ref, width, out_ref
):
    hidden = hidden_ref[...]
    upstream = mt(slope_ref[...], down_ref[...])
    scale = math.sqrt(2.0 / math.pi)
    curve = jnp.tanh(scale * (hidden + 0.044715 * (hidden * hidden * hidden)))
    steep = scale * (1.0 + (3.0 * 0.044715) * (hidden * hidden))
    hidden_slope = upstream * (
        0.5 * (1.0 + curve) + 0.5 * hidden * (1.0 - curve * curve) * steep
    )
    along = jnp.sum(hidden_slope * hidden, axis=-1, keepdims=True) * (1.0 / width)
    part = mt(hidden_slope.astype(BF16), latent_ref[...]) - along * embed_ref[...]
    part = (part / root_ref[...]).astype(BF16)
    half = part.shape[0]
    for chip in range(CHIPS):
        out_ref[chip, 0:half, :] = part
        out_ref[chip, half:, :] = reward_ref[...]


def stream_body(
    index_ref, half_ref, other_ref, label_ref, noise_ref, weight_ref, gain_ref, out_ref
):
    core = index_ref[0]
    first = index_ref[4]
    tokens = out_ref.shape[0]
    count = half_ref.shape[0]
    width = gain_ref.shape[1]
    token = lax.broadcasted_iota(jnp.int32, (tokens, 1), 0) + first
    own = label_ref[:, pl.ds(pl.multiple_of(core * count, count), count)]
    away = label_ref[:, pl.ds(pl.multiple_of((1 - core) * count, count), count)]
    own = (token == own).astype(F32).astype(BF16)
    away = (token == away).astype(F32).astype(BF16)
    every = (token == label_ref[...]).astype(F32).astype(BF16)
    noise = mm(every, noise_ref[...]).astype(BF16)
    inverse = mm(own, half_ref[:, width:]) + mm(away, other_ref[:, width:])
    inverse = jnp.sum(inverse, axis=-1, keepdims=True)
    unit = mm(own, half_ref[:, 0:width]) + mm(away, other_ref[:, 0:width])
    slope = mt(noise, weight_ref[...]) * gain_ref[...]
    mean = jnp.mean(slope, axis=-1, keepdims=True)
    along = jnp.mean(slope * unit, axis=-1, keepdims=True)
    out_ref[...] = ((slope - mean - unit * along) * inverse).astype(BF16)


def plan(noise_step):
    phase = (noise_step.astype(F32) / 1000.0 + 0.008) / 1.008 * (math.pi / 2.0)
    signal_root = jnp.cos(phase)
    return (signal_root, jnp.sqrt(1.0 - signal_root * signal_root))


def step(
    stream,
    queries,
    keys,
    values,
    clip_lengths,
    mod_shift,
    mod_scale,
    out_weight,
    final_weight,
    noisy_latents,
    timestep,
    crop_map,
    embed_weight,
    pre_gain,
    up_weight,
    down_weight,
    post_gain,
    head_weight,
):
    tokens = queries.shape[1]
    width = stream.shape[2]
    crop = crop_map[0]
    rows = crop.shape[0]
    half = rows // 2
    share = half // CHIPS
    core = lax.axis_index("core")
    zh = lax.axis_index("zh")
    y = lax.axis_index("y")
    chip = zh * 4 + y
    place = y * 2 + zh
    core_scalar = jnp.reshape(core, (1,)).astype(jnp.int32)
    own_first = (chip * 2 + core) * tokens
    spots = jnp.stack([core, zh, y, place, own_first]).astype(jnp.int32)

    near, across = lax.axis_size("zl"), lax.axis_size("x")
    by_zl = jnp.stack(ring_blocks(out_weight, "zl"))
    weight_blocks = ring_blocks(by_zl, "x")
    pair_blocks = [swap(block) for block in weight_blocks]
    up_pair = jnp.concatenate([up_weight, swap(up_weight)], axis=1)
    down_pair = jnp.concatenate([down_weight, swap(down_weight)], axis=0)

    (sent,) = kernel_call(
        pack_body,
        [((CHIPS, tokens, 4 * HEAD), BF16)],
        10**6,
        2 * MIB,
        [queries[0], keys[0], values[0]],
        spots,
    )
    mine = exchange(sent, CHIP).reshape(CHIPS * tokens, 4 * HEAD)
    other = swap(mine)
    spot_at = jnp.arange(2 * CHIPS * tokens, dtype=jnp.int32)
    spot_core = jnp.where(spot_at < CHIPS * tokens, core, 1 - core)
    spot_rest = spot_at % (CHIPS * tokens)
    token_at = (spot_rest // tokens) * (2 * tokens) + spot_core * tokens + spot_rest % tokens
    live = (token_at < clip_lengths[0]).astype(jnp.int32)[None]
    crop_core = (crop // tokens) % 2
    crop_at = (
        jnp.where(crop_core == core, 0, CHIPS * tokens)
        + (crop // (2 * tokens)) * tokens
        + crop % tokens
    )

    attended, weights, denominator = kernel_call(
        attend_body,
        [((rows, HEAD), BF16), ((rows, 2 * CHIPS * tokens), BF16), ((rows, 1), F32)],
        6 * 10**8,
        4 * MIB,
        [mine, other, crop_at[:, None], live],
    )

    indices = jnp.stack([core, chip, lax.axis_index("x"), lax.axis_index("zl")]).astype(jnp.int32)
    partial, own_weight = kernel_call(
        functools.partial(project_body, near, across),
        [((half, width + PATCH), BF16), ((out_weight.shape[0], width), BF16)],
        6 * 10**8,
        7 * MIB,
        [attended, swap(attended), crop[:, None]]
        + weight_blocks
        + pair_blocks
        + [stream[0], swap(stream[0]), noisy_latents[0], swap(noisy_latents[0])],
        indices,
    )
    arrived = exchange(partial.reshape(4, 2 * share, width + PATCH), "y")
    keep, give = kernel_call(
        partial_body,
        [((share, width + PATCH), F32), ((share, width + PATCH), BF16)],
        10**6,
        2 * MIB,
        [arrived],
        spots,
    )
    got = swap(give, "zh")
    signal_root, noise_root = plan(timestep[0])
    gain_rows = 1.0 + mod_scale[0]
    crop_copies, unit_own = kernel_call(
        layer_body,
        [((CHIPS, share, PATCH), BF16), ((share, width + PATCH), BF16)],
        2 * 10**7,
        2 * MIB,
        [
            keep,
            got,
            gain_rows[None],
            mod_shift,
            final_weight,
            jnp.broadcast_to(signal_root, (1, PATCH)),
            jnp.broadcast_to(noise_root, (1, PATCH)),
        ],
    )
    crop_tokens = exchange(crop_copies, ROWS).reshape(half, PATCH)

    unit_got = swap(unit_own, "zh")
    (unit_pair,) = kernel_call(
        pair_body,
        [((2 * share, width + PATCH), BF16)],
        10**6,
        MIB // 2,
        [unit_own, unit_got],
        spots,
    )
    unit_blocks = ring_blocks(unit_pair, "y")
    (unit_half,) = kernel_call(
        half_body, [((half, width + PATCH), BF16)], 10**6, 2 * MIB, unit_blocks, spots
    )
    unit_other = swap(unit_half)

    embedded = mm(crop_tokens, embed_weight)
    first_root = jnp.sqrt(jnp.mean(embedded * embedded, axis=-1, keepdims=True) + EPSILON)
    first_unit = embedded / first_root
    normed = (first_unit * pre_gain).astype(BF16)
    hidden = mm(normed, up_pair)
    active = jax.nn.gelu(hidden, approximate=True).astype(BF16)
    lowered = mm(active, down_pair).astype(BF16).reshape(CHIPS, share, -1)
    added = exchange(lowered, ROWS)
    reward_width = embedded.shape[1]
    slope_copies, reward_lanes = kernel_call(
        norm_body,
        [((CHIPS, share, reward_width), BF16), ((48, PATCH), BF16)],
        10**6,
        MIB,
        [embedded, added, post_gain[None], head_weight[None]],
        spots,
    )
    slope_half = exchange(slope_copies, ROWS).reshape(half, reward_width)
    gained_embed = (embed_weight.astype(F32) * pre_gain).astype(BF16)
    hidden_embed = mm(gained_embed, up_pair).astype(BF16)
    unit_embed = mt(first_unit.astype(BF16), embed_weight)
    (part_copies,) = kernel_call(
        lambda *refs: back_body(*refs[:-1], reward_width, refs[-1]),
        [((CHIPS, half + 48, PATCH), BF16)],
        3 * 10**8,
        4 * MIB,
        [slope_half, down_pair, hidden, hidden_embed, unit_embed, first_root, reward_lanes],
    )
    parts = exchange(part_copies, ROWS).astype(F32).sum(axis=0)
    direct = lax.optimization_barrier(mt(slope_half, embed_weight))
    direct = jnp.concatenate([direct, jnp.zeros((48, PATCH), F32)], axis=0)
    both = parts + direct
    back = swap(both)
    reward = both + back
    reward = reward[half, 0] + reward[half + 16, 0] + reward[half + 32, 0]
    same = crop[:, None] == crop[None, :]
    gained = final_weight.astype(F32) * gain_rows[:, None]
    gained16 = gained.astype(BF16)
    weight_latent = mm(own_weight, gained16)
    weight_sum = jnp.sum(own_weight.astype(F32), axis=1)
    unit_weight, unit_latent, row_inverse = kernel_call(
        unit_body,
        [((rows, HEAD), F32), ((rows, PATCH), F32), ((rows, 1), F32)],
        6 * 10**8,
        4 * MIB,
        [unit_half, unit_other, own_weight, gained16],
        spots,
    )
    query_slope, noise_slope = kernel_call(
        slope_body,
        [((rows, HEAD), BF16), ((rows, PATCH), BF16)],
        6 * 10**8,
        5 * MIB,
        [
            jnp.broadcast_to(-(noise_root / signal_root), (1, PATCH)),
            both,
            back,
            crop[:, None],
            crop[None, :],
            weight_latent.astype(BF16),
            jnp.mean(gained, axis=0)[None],
            weight_sum[None],
            unit_weight,
            unit_latent,
            row_inverse,
            attended,
            weights,
            denominator,
            mine,
            other,
        ],
        core_scalar,
    )

    earlier = same & (jnp.arange(rows)[None, :] < jnp.arange(rows)[:, None])
    first_seen = jnp.logical_not(jnp.any(earlier, axis=1))
    label = jnp.where(first_seen, crop, -1)
    (spread,) = kernel_call(
        spread_body,
        [((CHIPS, tokens, 2 * HEAD), BF16)],
        10**8,
        MIB,
        [query_slope, swap(query_slope), label[None]],
        core_scalar,
    )
    home = exchange(spread, CHIP)
    (grad_queries,) = kernel_call(home_body, [((tokens, HEADS * HEAD), BF16)], 10**6, MIB, [home])
    (grad_stream,) = kernel_call(
        stream_body,
        [((tokens, width), BF16)],
        6 * 10**8,
        5 * MIB,
        [unit_half, unit_other, label[None], noise_slope, final_weight, gain_rows[None]],
        spots,
    )
    return (jnp.reshape(reward, (1,)), grad_stream[None], grad_queries[None])


DP = ("x", "zl")
CTX = ("zh", "y", "core")


def solution(mesh):
    across = mesh.shape["dp"]
    near = min(4, across)
    fine = Mesh(
        mesh.devices.reshape(across // near, near, 2, 4, 2), ("x", "zl", "zh", "y", "core")
    )
    return jax.shard_map(
        step,
        mesh=fine,
        in_specs=(
            P(DP, CTX, None),
            P(DP, CTX, None),
            P(DP, CTX, None),
            P(DP, CTX, None),
            P(DP),
            P(DP, None),
            P(DP, None),
            P(CTX, DP),
            P(),
            P(DP, CTX, None),
            P(DP),
            P(DP, None),
            P(),
            P(),
            P(None, CTX),
            P(CTX, None),
            P(),
            P(),
        ),
        out_specs=(P(DP), P(DP, CTX, None), P(DP, CTX, None)),
        check_vma=False,
    )
```

```python
import functools
import math

import jax
import jax.numpy as jnp
from jax import lax
from jax.experimental import pallas as pl
from jax.experimental.pallas import tpu as pltpu
from jax.sharding import Mesh, PartitionSpec as P


HEADS = 16
HEAD = 128
PATCH = 128
CHIPS = 8

MASKED = -1e30
LOSS_SCALE = 16.0
EPSILON = 1e-06

F32 = jnp.float32
BF16 = jnp.bfloat16
CHIP = ("zh", "y")
ROWS = ("y", "zh")
MIB = 1024 * 1024


def dot(a, b, dims):
    return lax.dot_general(a, b, (dims, ((), ())), preferred_element_type=F32)


def mm(a, b):
    return dot(a, b, ((1,), (0,)))


def mt(a, b):
    return dot(a, b, ((1,), (1,)))


def exchange(pieces, axis):
    return lax.all_to_all(pieces, axis, split_axis=0, concat_axis=0, tiled=True)


def swap(value, axis="core"):
    return lax.ppermute(value, axis, [(0, 1), (1, 0)])


def ring_blocks(value, axis):
    size = lax.axis_size(axis)
    blocks = [value]
    for step in range(1, size):
        blocks.append(lax.ppermute(value, axis, [((i + step) % size, i) for i in range(size)]))
    return blocks


def whole(shape):
    return pl.BlockSpec(shape, lambda _: (0,) * len(shape))


def kernel_call(body, outs, flops, moved, operands, scalars=None, limit=None):
    specs = [whole(operand.shape) for operand in operands]
    if scalars is not None:
        specs = [pl.BlockSpec(memory_space=pltpu.SMEM)] + specs
        operands = [scalars] + operands
    return pl.pallas_call(
        body,
        grid=(1,),
        out_shape=[jax.ShapeDtypeStruct(shape, kind) for shape, kind in outs],
        in_specs=specs,
        out_specs=[whole(shape) for shape, _ in outs],
        compiler_params=pltpu.CompilerParams(vmem_limit_bytes=limit),
        cost_estimate=pl.CostEstimate(flops=flops, bytes_accessed=moved, transcendentals=0),
    )(*operands)


def pack_body(spots_ref, query_ref, key_ref, value_ref, out_ref):
    core = spots_ref[0]
    for chip in range(CHIPS):
        group = slice((chip // 2) * HEAD, (chip // 2 + 1) * HEAD)
        near = pl.multiple_of((2 * chip + core) * HEAD, HEAD)
        far = pl.multiple_of((2 * chip + 1 - core) * HEAD, HEAD)
        out_ref[chip, :, 0:HEAD] = query_ref[:, pl.ds(near, HEAD)]
        out_ref[chip, :, HEAD : 2 * HEAD] = query_ref[:, pl.ds(far, HEAD)]
        out_ref[chip, :, 2 * HEAD : 3 * HEAD] = key_ref[:, group]
        out_ref[chip, :, 3 * HEAD :] = value_ref[:, group]


def pick_rows(wanted, first, count):
    lanes = lax.broadcasted_iota(jnp.int32, (wanted.shape[0], count), 1) + first
    return (lanes == wanted).astype(F32).astype(BF16)


def attend_body(mine_ref, other_ref, at_ref, live_ref, att_ref, weights_ref, denominator_ref):
    span = mine_ref.shape[0]
    block = 128
    for start in range(0, at_ref.shape[0], block):
        here = slice(start, start + block)
        wanted = at_ref[here, :]
        query = mm(pick_rows(wanted, 0, span), mine_ref[:, 0:HEAD])
        query = query + mm(pick_rows(wanted, span, span), other_ref[:, HEAD : 2 * HEAD])
        query = query.astype(BF16)
        scale = 1.0 / math.sqrt(HEAD)
        first = mt(query, mine_ref[:, 2 * HEAD : 3 * HEAD]) * scale
        first = jnp.where(live_ref[:, 0:span] > 0, first, MASKED)
        second = mt(query, other_ref[:, 2 * HEAD : 3 * HEAD]) * scale
        second = jnp.where(live_ref[:, span:] > 0, second, MASKED)
        highest = jnp.maximum(
            jnp.max(first, axis=-1, keepdims=True), jnp.max(second, axis=-1, keepdims=True)
        )
        first = jnp.exp(first - highest)
        second = jnp.exp(second - highest)
        denominator = jnp.sum(first, axis=-1, keepdims=True) + jnp.sum(
            second, axis=-1, keepdims=True
        )
        first = first.astype(BF16)
        second = second.astype(BF16)
        blended = mm(first, mine_ref[:, 3 * HEAD :]) + mm(second, other_ref[:, 3 * HEAD :])
        att_ref[here, :] = (blended / denominator).astype(BF16)
        weights_ref[here, 0:span] = first
        weights_ref[here, span:] = second
        denominator_ref[here, :] = denominator


def project_body(near, across, index_ref, att_ref, att_other_ref, crop_ref, *refs):
    count = across
    own_refs, pair_refs, refs = refs[:count], refs[count : 2 * count], refs[2 * count :]
    stream_ref, stream_other_ref, noisy_ref, noisy_other_ref, out_ref, weight_ref = refs
    core, chip, x, zl = index_ref[0], index_ref[1], index_ref[2], index_ref[3]
    half = out_ref.shape[0]
    tokens = stream_ref.shape[0]
    width = stream_ref.shape[1]
    rows = pl.ds(pl.multiple_of(core * half, half), half)
    kept = att_ref[rows, :]
    other = att_other_ref[rows, :]
    wanted = crop_ref[rows, :] - chip * (2 * tokens)
    pick = pick_rows(wanted, core * tokens, tokens)
    pick_other = pick_rows(wanted, (1 - core) * tokens, tokens)
    for shift in range(across):
        for step in range(near):
            place = lax.rem(x + shift, across) * near + lax.rem(zl + step, near)
            size = own_refs[shift].shape[2]
            columns = pl.ds(pl.multiple_of(place * size, size), size)
            weight = own_refs[shift][step]
            weight_ref[:, columns] = weight
            total = mm(kept, weight) + mm(other, pair_refs[shift][step])
            total = total + mm(pick, stream_ref[:, columns])
            total = total + mm(pick_other, stream_other_ref[:, columns])
            out_ref[:, columns] = total.astype(BF16)
    noisy = mm(pick, noisy_ref[...]) + mm(pick_other, noisy_other_ref[...])
    out_ref[:, width:] = noisy.astype(BF16)


def slope_body(
    consts_ref,
    token_ref,
    back_ref,
    crop_ref,
    crop_row_ref,
    weight_latent_ref,
    mean_ref,
    sum_ref,
    unit_weight_ref,
    unit_latent_ref,
    inverse_ref,
    att_ref,
    weights_ref,
    denominator_ref,
    mine_ref,
    other_ref,
    out_ref,
    noise_ref,
):
    span = mine_ref.shape[0]
    block = 128
    core = consts_ref[3]
    half = out_ref.shape[0] // 2
    near, far = token_ref[0:half, :], back_ref[0:half, :]
    low = jnp.where(core == 0.0, near, far).astype(BF16)
    high = jnp.where(core == 0.0, far, near).astype(BF16)
    for start in range(0, out_ref.shape[0], block):
        here = slice(start, start + block)
        same = (crop_ref[here, :] == crop_row_ref[...]).astype(F32).astype(BF16)
        latent = mm(same[:, 0:half], low) + mm(same[:, half:], high)
        noise = (consts_ref[2] * latent).astype(BF16)
        noise_ref[here, :] = noise
        noise32 = noise.astype(F32)
        row_mean = jnp.sum(noise32 * mean_ref[...], axis=-1, keepdims=True)
        row_along = jnp.sum(noise32 * unit_latent_ref[here, :], axis=-1, keepdims=True)
        slope = mt(noise, weight_latent_ref[...]) - row_mean * sum_ref[...]
        slope = (slope - row_along * unit_weight_ref[here, :]) * inverse_ref[here, :]
        slope = slope.astype(BF16)
        delta = jnp.sum(slope.astype(F32) * att_ref[here, :].astype(F32), axis=-1, keepdims=True)
        recip = 1.0 / denominator_ref[here, :]
        first = mt(slope, mine_ref[:, 3 * HEAD :]) - delta
        first = (weights_ref[here, 0:span].astype(F32) * (first * recip)).astype(BF16)
        second = mt(slope, other_ref[:, 3 * HEAD :]) - delta
        second = (weights_ref[here, span:].astype(F32) * (second * recip)).astype(BF16)
        total = mm(first, mine_ref[:, 2 * HEAD : 3 * HEAD])
        total = total + mm(second, other_ref[:, 2 * HEAD : 3 * HEAD])
        out_ref[here, :] = (total * (1.0 / math.sqrt(HEAD))).astype(BF16)


def spread_body(core_ref, slope_ref, slope_other_ref, label_ref, out_ref):
    core = core_ref[0]
    tokens = out_ref.shape[1]
    own = slope_ref[...]
    other = slope_other_ref[...]
    left = jnp.where(core == 0, own, other)
    right = jnp.where(core == 0, other, own)
    for chip in range(CHIPS):
        token = lax.broadcasted_iota(jnp.int32, (tokens, 1), 0) + (2 * chip + core) * tokens
        pick = (token == label_ref[...]).astype(F32).astype(BF16)
        out_ref[chip, :, 0:HEAD] = mm(pick, left).astype(BF16)
        out_ref[chip, :, HEAD:] = mm(pick, right).astype(BF16)


def home_body(home_ref, out_ref):
    for chip in range(CHIPS):
        out_ref[:, chip * 2 * HEAD : (chip + 1) * 2 * HEAD] = home_ref[chip]


def partial_body(index_ref, arrived_ref, keep_ref, give_ref):
    zh = index_ref[1]
    share = keep_ref.shape[0]
    own = pl.ds(pl.multiple_of(zh * share, share), share)
    away = pl.ds(pl.multiple_of((1 - zh) * share, share), share)
    keep = arrived_ref[0, own, :].astype(F32)
    give = arrived_ref[0, away, :].astype(F32)
    for y in range(1, 4):
        keep = keep + arrived_ref[y, own, :].astype(F32)
        give = give + arrived_ref[y, away, :].astype(F32)
    keep_ref[...] = keep
    give_ref[...] = give.astype(BF16)


def split3(value):
    first = value.astype(BF16)
    rest = value - first.astype(F32)
    second = rest.astype(BF16)
    third = (rest - second.astype(F32)).astype(BF16)
    return first, second, third


def layer_body(consts_ref, keep_ref, got_ref, gain_ref, shift_ref, weight_ref, out_ref, unit_ref):
    width = gain_ref.shape[1]
    residual = keep_ref[:, 0:width] + got_ref[:, 0:width].astype(F32)
    noisy = keep_ref[:, width:] + got_ref[:, width:].astype(F32)
    centred = residual - jnp.mean(residual, axis=-1, keepdims=True)
    inverse = lax.rsqrt(jnp.mean(centred * centred, axis=-1, keepdims=True) + EPSILON)
    unit = centred * inverse
    modulated = (unit * gain_ref[...] + shift_ref[...]).astype(BF16)
    predicted = mm(modulated, weight_ref[...])
    denoised = ((noisy - consts_ref[1] * predicted) / consts_ref[0]).astype(BF16)
    for chip in range(CHIPS):
        out_ref[chip] = denoised
    unit_ref[:, 0:width] = unit.astype(BF16)
    lane = lax.broadcasted_iota(jnp.int32, noisy.shape, 1)
    tail = jnp.zeros(noisy.shape, F32)
    for place, piece in enumerate(split3(inverse)):
        tail = jnp.where(lane == place, piece.astype(F32), tail)
    unit_ref[:, width:] = tail.astype(BF16)


def pair_body(index_ref, own_ref, got_ref, out_ref):
    zh = index_ref[1]
    share = own_ref.shape[0]
    out_ref[pl.ds(pl.multiple_of(zh * share, share), share), :] = own_ref[...]
    out_ref[pl.ds(pl.multiple_of((1 - zh) * share, share), share), :] = got_ref[...]


def half_body(index_ref, *refs):
    y = index_ref[2]
    out_ref = refs[-1]
    size = refs[0].shape[0]
    for shift, ref in enumerate(refs[:-1]):
        place = lax.rem(y + shift, 4)
        out_ref[pl.ds(pl.multiple_of(place * size, size), size), :] = ref[...]


def unit_body(index_ref, half_ref, other_ref, head_ref, latent_ref, weight_ref, along_ref, inverse_ref):
    core = index_ref[0]
    count = half_ref.shape[0]
    width = head_ref.shape[1]
    for ref, place in ((half_ref, core), (other_ref, 1 - core)):
        here = pl.ds(pl.multiple_of(place * count, count), count)
        weight_ref[here, :] = mt(ref[:, 0:width], head_ref[...])
        along_ref[here, :] = mm(ref[:, 0:width], latent_ref[...]) * (1.0 / width)
        inverse_ref[here, :] = jnp.sum(ref[:, width:].astype(F32), axis=-1, keepdims=True)


def norm_body(index_ref, embedded_ref, added_ref, gain_ref, head_ref, out_ref, reward_ref):
    share = added_ref.shape[1]
    rows = 2 * embedded_ref.shape[0]
    own = pl.ds(pl.multiple_of(index_ref[3] * share, share), share)
    summed = added_ref[0].astype(F32)
    for chip in range(1, CHIPS):
        summed = summed + added_ref[chip].astype(F32)
    summed = embedded_ref[own, :] + summed
    root = jnp.sqrt(jnp.mean(summed * summed, axis=-1, keepdims=True) + EPSILON)
    unit = summed / root
    gain, head = gain_ref[...], head_ref[...]
    head_slope = -(LOSS_SCALE / rows) * head * gain
    slope = (head_slope - unit * jnp.mean(head_slope * unit, axis=-1, keepdims=True)) / root
    slope = slope.astype(BF16)
    for chip in range(CHIPS):
        out_ref[chip] = slope
    reward = jnp.sum(unit * gain * head, axis=-1, keepdims=True)
    reward = jnp.sum(reward, axis=0, keepdims=True) / rows
    lane = lax.broadcasted_iota(jnp.int32, reward_ref.shape, 1)
    tail = jnp.zeros(reward_ref.shape, F32)
    for place, piece in enumerate(split3(reward)):
        tail = jnp.where(lane == place, piece.astype(F32), tail)
    reward_ref[...] = tail.astype(BF16)


def back_body(
    slope_ref, down_ref, hidden_ref, latent_ref, embed_ref, root_ref, reward_ref, width, out_ref
):
    hidden = hidden_ref[...]
    upstream = mt(slope_ref[...], down_ref[...])
    scale = math.sqrt(2.0 / math.pi)
    curve = jnp.tanh(scale * (hidden + 0.044715 * (hidden * hidden * hidden)))
    steep = scale * (1.0 + (3.0 * 0.044715) * (hidden * hidden))
    hidden_slope = upstream * (
        0.5 * (1.0 + curve) + 0.5 * hidden * (1.0 - curve * curve) * steep
    )
    along = jnp.sum(hidden_slope * hidden, axis=-1, keepdims=True) * (1.0 / width)
    part = mt(hidden_slope.astype(BF16), latent_ref[...]) - along * embed_ref[...]
    part = (part / root_ref[...]).astype(BF16)
    half = part.shape[0]
    for chip in range(CHIPS):
        out_ref[chip, 0:half, :] = part
        out_ref[chip, half:, :] = reward_ref[...]


def stream_body(
    index_ref, half_ref, other_ref, label_ref, noise_ref, weight_ref, gain_ref, out_ref
):
    core = index_ref[0]
    first = index_ref[4]
    tokens = out_ref.shape[0]
    count = half_ref.shape[0]
    width = gain_ref.shape[1]
    token = lax.broadcasted_iota(jnp.int32, (tokens, 1), 0) + first
    own = label_ref[:, pl.ds(pl.multiple_of(core * count, count), count)]
    away = label_ref[:, pl.ds(pl.multiple_of((1 - core) * count, count), count)]
    own = (token == own).astype(F32).astype(BF16)
    away = (token == away).astype(F32).astype(BF16)
    every = (token == label_ref[...]).astype(F32).astype(BF16)
    noise = mm(every, noise_ref[...]).astype(BF16)
    inverse = mm(own, half_ref[:, width:]) + mm(away, other_ref[:, width:])
    inverse = jnp.sum(inverse, axis=-1, keepdims=True)
    unit = mm(own, half_ref[:, 0:width]) + mm(away, other_ref[:, 0:width])
    slope = mt(noise, weight_ref[...]) * gain_ref[...]
    mean = jnp.mean(slope, axis=-1, keepdims=True)
    along = jnp.mean(slope * unit, axis=-1, keepdims=True)
    out_ref[...] = ((slope - mean - unit * along) * inverse).astype(BF16)


def plan(noise_step):
    phase = (noise_step.astype(F32) / 1000.0 + 0.008) / 1.008 * (math.pi / 2.0)
    signal_root = jnp.cos(phase)
    return (signal_root, jnp.sqrt(1.0 - signal_root * signal_root))


def step(
    stream,
    queries,
    keys,
    values,
    clip_lengths,
    mod_shift,
    mod_scale,
    out_weight,
    final_weight,
    noisy_latents,
    timestep,
    crop_map,
    embed_weight,
    pre_gain,
    up_weight,
    down_weight,
    post_gain,
    head_weight,
):
    tokens = queries.shape[1]
    width = stream.shape[2]
    crop = crop_map[0]
    rows = crop.shape[0]
    half = rows // 2
    share = half // CHIPS
    core = lax.axis_index("core")
    zh = lax.axis_index("zh")
    y = lax.axis_index("y")
    chip = zh * 4 + y
    place = y * 2 + zh
    core_scalar = jnp.reshape(core, (1,)).astype(jnp.int32)
    own_first = (chip * 2 + core) * tokens
    spots = jnp.stack([core, zh, y, place, own_first]).astype(jnp.int32)

    near, across = lax.axis_size("zl"), lax.axis_size("x")
    by_zl = jnp.stack(ring_blocks(out_weight, "zl"))
    weight_blocks = ring_blocks(by_zl, "x")
    pair_blocks = [swap(block) for block in weight_blocks]
    up_pair = jnp.concatenate([up_weight, swap(up_weight)], axis=1)
    down_pair = jnp.concatenate([down_weight, swap(down_weight)], axis=0)

    stream_other = swap(stream[0])
    noisy_other = swap(noisy_latents[0])

    (sent,) = kernel_call(
        pack_body,
        [((CHIPS, tokens, 4 * HEAD), BF16)],
        10**6,
        2 * MIB,
        [queries[0], keys[0], values[0]],
        spots,
    )
    mine = exchange(sent, CHIP).reshape(CHIPS * tokens, 4 * HEAD)
    other = swap(mine)
    spot_at = jnp.arange(2 * CHIPS * tokens, dtype=jnp.int32)
    spot_core = jnp.where(spot_at < CHIPS * tokens, core, 1 - core)
    spot_rest = spot_at % (CHIPS * tokens)
    token_at = (spot_rest // tokens) * (2 * tokens) + spot_core * tokens + spot_rest % tokens
    live = (token_at < clip_lengths[0]).astype(jnp.int32)[None]
    crop_core = (crop // tokens) % 2
    crop_at = (
        jnp.where(crop_core == core, 0, CHIPS * tokens)
        + (crop // (2 * tokens)) * tokens
        + crop % tokens
    )
    same = crop[:, None] == crop[None, :]
    earlier = same & (jnp.arange(rows)[None, :] < jnp.arange(rows)[:, None])
    first_seen = jnp.logical_not(jnp.any(earlier, axis=1))
    label = jnp.where(first_seen, crop, -1)
    label = label[None]
    indices = jnp.stack([core, chip, lax.axis_index("x"), lax.axis_index("zl")]).astype(jnp.int32)
    signal_root, noise_root = plan(timestep[0])
    consts = jnp.stack(
        [signal_root, noise_root, -(noise_root / signal_root), core.astype(F32)]
    )
    gain_rows = 1.0 + mod_scale[0]
    gain_line = gain_rows[None]
    at_column = crop_at[:, None]

    attended, weights, denominator = kernel_call(
        attend_body,
        [((rows, HEAD), BF16), ((rows, 2 * CHIPS * tokens), BF16), ((rows, 1), F32)],
        6 * 10**8,
        4 * MIB,
        [mine, other, at_column, live],
        limit=24 * MIB,
    )

    partial, own_weight = kernel_call(
        functools.partial(project_body, near, across),
        [((half, width + PATCH), BF16), ((out_weight.shape[0], width), BF16)],
        6 * 10**8,
        7 * MIB,
        [attended, swap(attended), crop[:, None]]
        + weight_blocks
        + pair_blocks
        + [stream[0], stream_other, noisy_latents[0], noisy_other],
        indices,
    )
    arrived = exchange(partial.reshape(4, 2 * share, width + PATCH), "y")
    keep, give = kernel_call(
        partial_body,
        [((share, width + PATCH), F32), ((share, width + PATCH), BF16)],
        10**6,
        2 * MIB,
        [arrived],
        spots,
        limit=16 * MIB,
    )
    got = swap(give, "zh")
    crop_copies, unit_own = kernel_call(
        layer_body,
        [((CHIPS, share, PATCH), BF16), ((share, width + PATCH), BF16)],
        2 * 10**7,
        2 * MIB,
        [keep, got, gain_line, mod_shift, final_weight],
        consts,
    )
    crop_tokens = exchange(crop_copies, ROWS).reshape(half, PATCH)

    unit_got = swap(unit_own, "zh")
    (unit_pair,) = kernel_call(
        pair_body,
        [((2 * share, width + PATCH), BF16)],
        10**6,
        MIB // 2,
        [unit_own, unit_got],
        spots,
    )
    unit_blocks = ring_blocks(unit_pair, "y")
    (unit_half,) = kernel_call(
        half_body,
        [((half, width + PATCH), BF16)],
        10**6,
        2 * MIB,
        unit_blocks,
        spots,
        limit=16 * MIB,
    )
    unit_other = swap(unit_half)

    embedded = mm(crop_tokens, embed_weight)
    first_root = jnp.sqrt(jnp.mean(embedded * embedded, axis=-1, keepdims=True) + EPSILON)
    first_unit = embedded / first_root
    normed = (first_unit * pre_gain).astype(BF16)
    hidden = mm(normed, up_pair)
    active = jax.nn.gelu(hidden, approximate=True).astype(BF16)
    lowered = mm(active, down_pair).astype(BF16).reshape(CHIPS, share, -1)
    added = exchange(lowered, ROWS)
    reward_width = embedded.shape[1]
    slope_copies, reward_lanes = kernel_call(
        norm_body,
        [((CHIPS, share, reward_width), BF16), ((16, PATCH), BF16)],
        10**6,
        MIB,
        [embedded, added, post_gain[None], head_weight[None]],
        spots,
    )
    slope_half = exchange(slope_copies, ROWS).reshape(half, reward_width)
    gained_embed = (embed_weight.astype(F32) * pre_gain).astype(BF16)
    hidden_embed = mm(gained_embed, up_pair).astype(BF16)
    unit_embed = mt(first_unit.astype(BF16), embed_weight)
    (part_copies,) = kernel_call(
        lambda *refs: back_body(*refs[:-1], reward_width, refs[-1]),
        [((CHIPS, half + 16, PATCH), BF16)],
        3 * 10**8,
        4 * MIB,
        [slope_half, down_pair, hidden, hidden_embed, unit_embed, first_root, reward_lanes],
    )
    parts = exchange(part_copies, ROWS).astype(F32).sum(axis=0)
    direct = lax.optimization_barrier(mt(slope_half, embed_weight))
    direct = jnp.concatenate([direct, jnp.zeros((16, PATCH), F32)], axis=0)
    both = parts + direct
    back = swap(both)
    reward = both + back
    reward = reward[half, 0] + reward[half, 1] + reward[half, 2]
    gained = final_weight.astype(F32) * gain_rows[:, None]
    gained16 = gained.astype(BF16)
    weight_latent = mm(own_weight, gained16)
    weight_sum = jnp.sum(own_weight.astype(F32), axis=1)
    unit_weight, unit_latent, row_inverse = kernel_call(
        unit_body,
        [((rows, HEAD), F32), ((rows, PATCH), F32), ((rows, 1), F32)],
        6 * 10**8,
        4 * MIB,
        [unit_half, unit_other, own_weight, gained16],
        spots,
    )
    query_slope, noise_slope = kernel_call(
        slope_body,
        [((rows, HEAD), BF16), ((rows, PATCH), BF16)],
        6 * 10**8,
        5 * MIB,
        [
            both,
            back,
            crop[:, None],
            crop[None, :],
            weight_latent.astype(BF16),
            jnp.mean(gained, axis=0)[None],
            weight_sum[None],
            unit_weight,
            unit_latent,
            row_inverse,
            attended,
            weights,
            denominator,
            mine,
            other,
        ],
        consts,
    )

    (spread,) = kernel_call(
        spread_body,
        [((CHIPS, tokens, 2 * HEAD), BF16)],
        10**8,
        MIB,
        [query_slope, swap(query_slope), label],
        core_scalar,
        limit=16 * MIB,
    )
    home = exchange(spread, CHIP)
    (grad_queries,) = kernel_call(
        home_body, [((tokens, HEADS * HEAD), BF16)], 10**6, MIB, [home], limit=16 * MIB
    )
    (grad_stream,) = kernel_call(
        stream_body,
        [((tokens, width), BF16)],
        6 * 10**8,
        5 * MIB,
        [unit_half, unit_other, label, noise_slope, final_weight, gain_line],
        spots,
    )
    return (jnp.reshape(reward, (1,)), grad_stream[None], grad_queries[None])


DP = ("x", "zl")
CTX = ("zh", "y", "core")


def solution(mesh):
    across = mesh.shape["dp"]
    near = min(4, across)
    fine = Mesh(
        mesh.devices.reshape(across // near, near, 2, 4, 2), ("x", "zl", "zh", "y", "core")
    )
    return jax.shard_map(
        step,
        mesh=fine,
        in_specs=(
            P(DP, CTX, None),
            P(DP, CTX, None),
            P(DP, CTX, None),
            P(DP, CTX, None),
            P(DP),
            P(DP, None),
            P(DP, None),
            P(CTX, DP),
            P(),
            P(DP, CTX, None),
            P(DP),
            P(DP, None),
            P(),
            P(),
            P(None, CTX),
            P(CTX, None),
            P(),
            P(),
        ),
        out_specs=(P(DP), P(DP, CTX, None), P(DP, CTX, None)),
        check_vma=False,
    )
```

```python
import functools
import math

import jax
import jax.numpy as jnp
from jax import lax
from jax.experimental import pallas as pl
from jax.experimental.pallas import tpu as pltpu
from jax.sharding import Mesh, PartitionSpec as P


HEADS = 16
HEAD = 128
PATCH = 128
CHIPS = 8

MASKED = -1e30
LOSS_SCALE = 16.0
EPSILON = 1e-06

F32 = jnp.float32
BF16 = jnp.bfloat16
CHIP = ("zh", "y")
ROWS = ("y", "zh")
MIB = 1024 * 1024


def dot(a, b, dims):
    return lax.dot_general(a, b, (dims, ((), ())), preferred_element_type=F32)


def mm(a, b):
    return dot(a, b, ((1,), (0,)))


def mt(a, b):
    return dot(a, b, ((1,), (1,)))


def exchange(pieces, axis):
    return lax.all_to_all(pieces, axis, split_axis=0, concat_axis=0, tiled=True)


def swap(value, axis="core"):
    return lax.ppermute(value, axis, [(0, 1), (1, 0)])


def ring_blocks(value, axis):
    size = lax.axis_size(axis)
    blocks = [value]
    for step in range(1, size):
        blocks.append(lax.ppermute(value, axis, [((i + step) % size, i) for i in range(size)]))
    return blocks


def whole(shape):
    return pl.BlockSpec(shape, lambda _: (0,) * len(shape))


def kernel_call(body, outs, flops, moved, operands, scalars=None, limit=None):
    specs = [whole(operand.shape) for operand in operands]
    if scalars is not None:
        specs = [pl.BlockSpec(memory_space=pltpu.SMEM)] + specs
        operands = [scalars] + operands
    return pl.pallas_call(
        body,
        grid=(1,),
        out_shape=[jax.ShapeDtypeStruct(shape, kind) for shape, kind in outs],
        in_specs=specs,
        out_specs=[whole(shape) for shape, _ in outs],
        compiler_params=pltpu.CompilerParams(vmem_limit_bytes=limit),
        cost_estimate=pl.CostEstimate(flops=flops, bytes_accessed=moved, transcendentals=0),
    )(*operands)


def pack_body(spots_ref, query_ref, key_ref, value_ref, out_ref):
    core = spots_ref[0]
    for chip in range(CHIPS):
        group = slice((chip // 2) * HEAD, (chip // 2 + 1) * HEAD)
        near = pl.multiple_of((2 * chip + core) * HEAD, HEAD)
        far = pl.multiple_of((2 * chip + 1 - core) * HEAD, HEAD)
        out_ref[chip, :, 0:HEAD] = query_ref[:, pl.ds(near, HEAD)]
        out_ref[chip, :, HEAD : 2 * HEAD] = query_ref[:, pl.ds(far, HEAD)]
        out_ref[chip, :, 2 * HEAD : 3 * HEAD] = key_ref[:, group]
        out_ref[chip, :, 3 * HEAD :] = value_ref[:, group]


def pick_rows(wanted, first, count):
    lanes = lax.broadcasted_iota(jnp.int32, (wanted.shape[0], count), 1) + first
    return (lanes == wanted).astype(F32).astype(BF16)


def attend_body(mine_ref, other_ref, at_ref, live_ref, att_ref, weights_ref, denominator_ref):
    span = mine_ref.shape[0]
    block = 128
    for start in range(0, at_ref.shape[0], block):
        here = slice(start, start + block)
        wanted = at_ref[here, :]
        query = mm(pick_rows(wanted, 0, span), mine_ref[:, 0:HEAD])
        query = query + mm(pick_rows(wanted, span, span), other_ref[:, HEAD : 2 * HEAD])
        query = query.astype(BF16)
        scale = 1.0 / math.sqrt(HEAD)
        first = mt(query, mine_ref[:, 2 * HEAD : 3 * HEAD]) * scale
        first = jnp.where(live_ref[:, 0:span] > 0, first, MASKED)
        second = mt(query, other_ref[:, 2 * HEAD : 3 * HEAD]) * scale
        second = jnp.where(live_ref[:, span:] > 0, second, MASKED)
        highest = jnp.maximum(
            jnp.max(first, axis=-1, keepdims=True), jnp.max(second, axis=-1, keepdims=True)
        )
        first = jnp.exp(first - highest)
        second = jnp.exp(second - highest)
        denominator = jnp.sum(first, axis=-1, keepdims=True) + jnp.sum(
            second, axis=-1, keepdims=True
        )
        first = first.astype(BF16)
        second = second.astype(BF16)
        blended = mm(first, mine_ref[:, 3 * HEAD :]) + mm(second, other_ref[:, 3 * HEAD :])
        att_ref[here, :] = (blended / denominator).astype(BF16)
        weights_ref[here, 0:span] = first
        weights_ref[here, span:] = second
        denominator_ref[here, :] = denominator


def project_body(near, across, index_ref, att_ref, att_other_ref, crop_ref, *refs):
    count = across
    own_refs, pair_refs, refs = refs[:count], refs[count : 2 * count], refs[2 * count :]
    stream_ref, stream_other_ref, noisy_ref, noisy_other_ref, out_ref, weight_ref = refs
    core, chip, x, zl = index_ref[0], index_ref[1], index_ref[2], index_ref[3]
    half = out_ref.shape[0]
    tokens = stream_ref.shape[0]
    width = stream_ref.shape[1]
    rows = pl.ds(pl.multiple_of(core * half, half), half)
    kept = att_ref[rows, :]
    other = att_other_ref[rows, :]
    wanted = crop_ref[rows, :] - chip * (2 * tokens)
    pick = pick_rows(wanted, core * tokens, tokens)
    pick_other = pick_rows(wanted, (1 - core) * tokens, tokens)
    for shift in range(across):
        for step in range(near):
            place = lax.rem(x + shift, across) * near + lax.rem(zl + step, near)
            size = own_refs[shift].shape[2]
            columns = pl.ds(pl.multiple_of(place * size, size), size)
            weight = own_refs[shift][step]
            weight_ref[:, columns] = weight
            total = mm(kept, weight) + mm(other, pair_refs[shift][step])
            total = total + mm(pick, stream_ref[:, columns])
            total = total + mm(pick_other, stream_other_ref[:, columns])
            out_ref[:, columns] = total.astype(BF16)
    noisy = mm(pick, noisy_ref[...]) + mm(pick_other, noisy_other_ref[...])
    out_ref[:, width:] = noisy.astype(BF16)


def slope_body(
    consts_ref,
    token_ref,
    back_ref,
    crop_ref,
    crop_row_ref,
    weight_latent_ref,
    mean_ref,
    sum_ref,
    unit_weight_ref,
    unit_latent_ref,
    inverse_ref,
    att_ref,
    weights_ref,
    denominator_ref,
    mine_ref,
    other_ref,
    out_ref,
    noise_ref,
):
    span = mine_ref.shape[0]
    block = 128
    core = consts_ref[3]
    half = out_ref.shape[0] // 2
    near, far = token_ref[0:half, :], back_ref[0:half, :]
    low = jnp.where(core == 0.0, near, far).astype(BF16)
    high = jnp.where(core == 0.0, far, near).astype(BF16)
    for start in range(0, out_ref.shape[0], block):
        here = slice(start, start + block)
        same = (crop_ref[here, :] == crop_row_ref[...]).astype(F32).astype(BF16)
        latent = mm(same[:, 0:half], low) + mm(same[:, half:], high)
        noise = (consts_ref[2] * latent).astype(BF16)
        noise_ref[here, :] = noise
        noise32 = noise.astype(F32)
        row_mean = jnp.sum(noise32 * mean_ref[...], axis=-1, keepdims=True)
        row_along = jnp.sum(noise32 * unit_latent_ref[here, :], axis=-1, keepdims=True)
        slope = mt(noise, weight_latent_ref[...]) - row_mean * sum_ref[...]
        slope = (slope - row_along * unit_weight_ref[here, :]) * inverse_ref[here, :]
        slope = slope.astype(BF16)
        delta = jnp.sum(slope.astype(F32) * att_ref[here, :].astype(F32), axis=-1, keepdims=True)
        recip = 1.0 / denominator_ref[here, :]
        first = mt(slope, mine_ref[:, 3 * HEAD :]) - delta
        first = (weights_ref[here, 0:span].astype(F32) * (first * recip)).astype(BF16)
        second = mt(slope, other_ref[:, 3 * HEAD :]) - delta
        second = (weights_ref[here, span:].astype(F32) * (second * recip)).astype(BF16)
        total = mm(first, mine_ref[:, 2 * HEAD : 3 * HEAD])
        total = total + mm(second, other_ref[:, 2 * HEAD : 3 * HEAD])
        out_ref[here, :] = (total * (1.0 / math.sqrt(HEAD))).astype(BF16)


def spread_body(core_ref, slope_ref, slope_other_ref, label_ref, out_ref):
    core = core_ref[0]
    tokens = out_ref.shape[1]
    own = slope_ref[...]
    other = slope_other_ref[...]
    left = jnp.where(core == 0, own, other)
    right = jnp.where(core == 0, other, own)
    for chip in range(CHIPS):
        token = lax.broadcasted_iota(jnp.int32, (tokens, 1), 0) + (2 * chip + core) * tokens
        pick = (token == label_ref[...]).astype(F32).astype(BF16)
        out_ref[chip, :, 0:HEAD] = mm(pick, left).astype(BF16)
        out_ref[chip, :, HEAD:] = mm(pick, right).astype(BF16)


def home_body(home_ref, out_ref):
    for chip in range(CHIPS):
        out_ref[:, chip * 2 * HEAD : (chip + 1) * 2 * HEAD] = home_ref[chip]


def partial_body(index_ref, arrived_ref, keep_ref, give_ref):
    zh = index_ref[1]
    share = keep_ref.shape[0]
    own = pl.ds(pl.multiple_of(zh * share, share), share)
    away = pl.ds(pl.multiple_of((1 - zh) * share, share), share)
    keep = arrived_ref[0, own, :].astype(F32)
    give = arrived_ref[0, away, :].astype(F32)
    for y in range(1, 4):
        keep = keep + arrived_ref[y, own, :].astype(F32)
        give = give + arrived_ref[y, away, :].astype(F32)
    keep_ref[...] = keep
    give_ref[...] = give.astype(BF16)


def split3(value):
    first = value.astype(BF16)
    rest = value - first.astype(F32)
    second = rest.astype(BF16)
    third = (rest - second.astype(F32)).astype(BF16)
    return first, second, third


def layer_body(consts_ref, keep_ref, got_ref, gain_ref, shift_ref, weight_ref, out_ref, unit_ref):
    width = gain_ref.shape[1]
    residual = keep_ref[:, 0:width] + got_ref[:, 0:width].astype(F32)
    noisy = keep_ref[:, width:] + got_ref[:, width:].astype(F32)
    centred = residual - jnp.mean(residual, axis=-1, keepdims=True)
    inverse = lax.rsqrt(jnp.mean(centred * centred, axis=-1, keepdims=True) + EPSILON)
    unit = centred * inverse
    modulated = (unit * gain_ref[...] + shift_ref[...]).astype(BF16)
    predicted = mm(modulated, weight_ref[...])
    denoised = ((noisy - consts_ref[1] * predicted) / consts_ref[0]).astype(BF16)
    for chip in range(CHIPS):
        out_ref[chip] = denoised
    unit_ref[:, 0:width] = unit.astype(BF16)
    lane = lax.broadcasted_iota(jnp.int32, noisy.shape, 1)
    tail = jnp.zeros(noisy.shape, F32)
    for place, piece in enumerate(split3(inverse)):
        tail = jnp.where(lane == place, piece.astype(F32), tail)
    unit_ref[:, width:] = tail.astype(BF16)


def pair_body(index_ref, own_ref, got_ref, out_ref):
    zh = index_ref[1]
    share = own_ref.shape[0]
    out_ref[pl.ds(pl.multiple_of(zh * share, share), share), :] = own_ref[...]
    out_ref[pl.ds(pl.multiple_of((1 - zh) * share, share), share), :] = got_ref[...]


def half_body(index_ref, *refs):
    y = index_ref[2]
    out_ref = refs[-1]
    size = refs[0].shape[0]
    for shift, ref in enumerate(refs[:-1]):
        place = lax.rem(y + shift, 4)
        out_ref[pl.ds(pl.multiple_of(place * size, size), size), :] = ref[...]


def unit_body(index_ref, half_ref, other_ref, head_ref, latent_ref, weight_ref, along_ref, inverse_ref):
    core = index_ref[0]
    count = half_ref.shape[0]
    width = head_ref.shape[1]
    for ref, place in ((half_ref, core), (other_ref, 1 - core)):
        here = pl.ds(pl.multiple_of(place * count, count), count)
        weight_ref[here, :] = mt(ref[:, 0:width], head_ref[...])
        along_ref[here, :] = mm(ref[:, 0:width], latent_ref[...]) * (1.0 / width)
        inverse_ref[here, :] = jnp.sum(ref[:, width:].astype(F32), axis=-1, keepdims=True)


def norm_body(index_ref, embedded_ref, added_ref, gain_ref, head_ref, out_ref, reward_ref):
    share = added_ref.shape[1]
    rows = 2 * embedded_ref.shape[0]
    own = pl.ds(pl.multiple_of(index_ref[3] * share, share), share)
    summed = added_ref[0].astype(F32)
    for chip in range(1, CHIPS):
        summed = summed + added_ref[chip].astype(F32)
    summed = embedded_ref[own, :] + summed
    root = jnp.sqrt(jnp.mean(summed * summed, axis=-1, keepdims=True) + EPSILON)
    unit = summed / root
    gain, head = gain_ref[...], head_ref[...]
    head_slope = -(LOSS_SCALE / rows) * head * gain
    slope = (head_slope - unit * jnp.mean(head_slope * unit, axis=-1, keepdims=True)) / root
    slope = slope.astype(BF16)
    for chip in range(CHIPS):
        out_ref[chip] = slope
    reward = jnp.sum(unit * gain * head, axis=-1, keepdims=True)
    reward = jnp.sum(reward, axis=0, keepdims=True) / rows
    lane = lax.broadcasted_iota(jnp.int32, reward_ref.shape, 1)
    tail = jnp.zeros(reward_ref.shape, F32)
    for place, piece in enumerate(split3(reward)):
        tail = jnp.where(lane == place, piece.astype(F32), tail)
    reward_ref[...] = tail.astype(BF16)


def back_body(
    slope_ref, down_ref, hidden_ref, latent_ref, embed_ref, root_ref, reward_ref, width, out_ref
):
    hidden = hidden_ref[...]
    upstream = mt(slope_ref[...], down_ref[...])
    scale = math.sqrt(2.0 / math.pi)
    curve = jnp.tanh(scale * (hidden + 0.044715 * (hidden * hidden * hidden)))
    steep = scale * (1.0 + (3.0 * 0.044715) * (hidden * hidden))
    hidden_slope = upstream * (
        0.5 * (1.0 + curve) + 0.5 * hidden * (1.0 - curve * curve) * steep
    )
    along = jnp.sum(hidden_slope * hidden, axis=-1, keepdims=True) * (1.0 / width)
    part = mt(hidden_slope.astype(BF16), latent_ref[...]) - along * embed_ref[...]
    part = (part / root_ref[...]).astype(BF16)
    half = part.shape[0]
    for chip in range(CHIPS):
        out_ref[chip, 0:half, :] = part
        out_ref[chip, half:, :] = reward_ref[...]


def stream_body(
    index_ref, half_ref, other_ref, label_ref, noise_ref, weight_ref, gain_ref, out_ref
):
    core = index_ref[0]
    first = index_ref[4]
    tokens = out_ref.shape[0]
    count = half_ref.shape[0]
    width = gain_ref.shape[1]
    token = lax.broadcasted_iota(jnp.int32, (tokens, 1), 0) + first
    own = label_ref[:, pl.ds(pl.multiple_of(core * count, count), count)]
    away = label_ref[:, pl.ds(pl.multiple_of((1 - core) * count, count), count)]
    own = (token == own).astype(F32).astype(BF16)
    away = (token == away).astype(F32).astype(BF16)
    every = (token == label_ref[...]).astype(F32).astype(BF16)
    noise = mm(every, noise_ref[...]).astype(BF16)
    inverse = mm(own, half_ref[:, width:]) + mm(away, other_ref[:, width:])
    inverse = jnp.sum(inverse, axis=-1, keepdims=True)
    unit = mm(own, half_ref[:, 0:width]) + mm(away, other_ref[:, 0:width])
    slope = mt(noise, weight_ref[...]) * gain_ref[...]
    mean = jnp.mean(slope, axis=-1, keepdims=True)
    along = jnp.mean(slope * unit, axis=-1, keepdims=True)
    out_ref[...] = ((slope - mean - unit * along) * inverse).astype(BF16)


def plan(noise_step):
    phase = (noise_step.astype(F32) / 1000.0 + 0.008) / 1.008 * (math.pi / 2.0)
    signal_root = jnp.cos(phase)
    return (signal_root, jnp.sqrt(1.0 - signal_root * signal_root))


def step(
    stream,
    queries,
    keys,
    values,
    clip_lengths,
    mod_shift,
    mod_scale,
    out_weight,
    final_weight,
    noisy_latents,
    timestep,
    crop_map,
    embed_weight,
    pre_gain,
    up_weight,
    down_weight,
    post_gain,
    head_weight,
):
    tokens = queries.shape[1]
    width = stream.shape[2]
    crop = crop_map[0]
    rows = crop.shape[0]
    half = rows // 2
    share = half // CHIPS
    core = lax.axis_index("core")
    zh = lax.axis_index("zh")
    y = lax.axis_index("y")
    chip = zh * 4 + y
    place = y * 2 + zh
    core_scalar = jnp.reshape(core, (1,)).astype(jnp.int32)
    own_first = (chip * 2 + core) * tokens
    spots = jnp.stack([core, zh, y, place, own_first]).astype(jnp.int32)

    near, across = lax.axis_size("zl"), lax.axis_size("x")
    by_zl = jnp.stack(ring_blocks(out_weight, "zl"))
    weight_blocks = ring_blocks(by_zl, "x")
    pair_blocks = [swap(block) for block in weight_blocks]
    up_pair = jnp.concatenate([up_weight, swap(up_weight)], axis=1)
    down_pair = jnp.concatenate([down_weight, swap(down_weight)], axis=0)

    stream_other = swap(stream[0])
    noisy_other = swap(noisy_latents[0])

    (sent,) = kernel_call(
        pack_body,
        [((CHIPS, tokens, 4 * HEAD), BF16)],
        10**6,
        2 * MIB,
        [queries[0], keys[0], values[0]],
        core_scalar,
    )
    mine = exchange(sent, CHIP).reshape(CHIPS * tokens, 4 * HEAD)
    other = swap(mine)
    spot_at = jnp.arange(2 * CHIPS * tokens, dtype=jnp.int32)
    spot_core = jnp.where(spot_at < CHIPS * tokens, core, 1 - core)
    spot_rest = spot_at % (CHIPS * tokens)
    token_at = (spot_rest // tokens) * (2 * tokens) + spot_core * tokens + spot_rest % tokens
    live = (token_at < clip_lengths[0]).astype(jnp.int32)[None]
    crop_core = (crop // tokens) % 2
    crop_at = (
        jnp.where(crop_core == core, 0, CHIPS * tokens)
        + (crop // (2 * tokens)) * tokens
        + crop % tokens
    )
    same = crop[:, None] == crop[None, :]
    earlier = same & (jnp.arange(rows)[None, :] < jnp.arange(rows)[:, None])
    first_seen = jnp.logical_not(jnp.any(earlier, axis=1))
    label = jnp.where(first_seen, crop, -1)
    label = label[None]
    indices = jnp.stack([core, chip, lax.axis_index("x"), lax.axis_index("zl")]).astype(jnp.int32)
    signal_root, noise_root = plan(timestep[0])
    consts = jnp.stack(
        [signal_root, noise_root, -(noise_root / signal_root), core.astype(F32)]
    )
    gain_rows = 1.0 + mod_scale[0]
    gain_line = gain_rows[None]
    at_column = crop_at[:, None]

    attended, weights, denominator = kernel_call(
        attend_body,
        [((rows, HEAD), BF16), ((rows, 2 * CHIPS * tokens), BF16), ((rows, 1), F32)],
        6 * 10**8,
        4 * MIB,
        [mine, other, at_column, live],
        limit=24 * MIB,
    )

    partial, own_weight = kernel_call(
        functools.partial(project_body, near, across),
        [((half, width + PATCH), BF16), ((out_weight.shape[0], width), BF16)],
        6 * 10**8,
        7 * MIB,
        [attended, swap(attended), crop[:, None]]
        + weight_blocks
        + pair_blocks
        + [stream[0], stream_other, noisy_latents[0], noisy_other],
        indices,
    )
    arrived = exchange(partial.reshape(4, 2 * share, width + PATCH), "y")
    keep, give = kernel_call(
        partial_body,
        [((share, width + PATCH), F32), ((share, width + PATCH), BF16)],
        10**6,
        2 * MIB,
        [arrived],
        spots,
        limit=16 * MIB,
    )
    got = swap(give, "zh")
    crop_copies, unit_own = kernel_call(
        layer_body,
        [((CHIPS, share, PATCH), BF16), ((share, width + PATCH), BF16)],
        2 * 10**7,
        2 * MIB,
        [keep, got, gain_line, mod_shift, final_weight],
        consts,
    )
    crop_tokens = exchange(crop_copies, ROWS).reshape(half, PATCH)

    unit_got = swap(unit_own, "zh")
    (unit_pair,) = kernel_call(
        pair_body,
        [((2 * share, width + PATCH), BF16)],
        10**6,
        MIB // 2,
        [unit_own, unit_got],
        spots,
    )
    unit_blocks = ring_blocks(unit_pair, "y")
    (unit_half,) = kernel_call(
        half_body,
        [((half, width + PATCH), BF16)],
        10**6,
        2 * MIB,
        unit_blocks,
        spots,
        limit=16 * MIB,
    )
    unit_other = swap(unit_half)

    gained = final_weight.astype(F32) * gain_rows[:, None]
    gained16 = gained.astype(BF16)
    weight_latent = mm(own_weight, gained16)
    weight_sum = jnp.sum(own_weight.astype(F32), axis=1)
    weight_latent = weight_latent.astype(BF16)
    mean_line = jnp.mean(gained, axis=0)[None]
    sum_line = weight_sum[None]
    post_line = post_gain[None]
    head_line = head_weight[None]

    embedded = mm(crop_tokens, embed_weight)
    first_root = jnp.sqrt(jnp.mean(embedded * embedded, axis=-1, keepdims=True) + EPSILON)
    first_unit = embedded / first_root
    normed = (first_unit * pre_gain).astype(BF16)
    hidden = mm(normed, up_pair)
    active = jax.nn.gelu(hidden, approximate=True).astype(BF16)
    lowered = mm(active, down_pair).astype(BF16).reshape(CHIPS, share, -1)
    added = exchange(lowered, ROWS)
    reward_width = embedded.shape[1]
    slope_copies, reward_lanes = kernel_call(
        norm_body,
        [((CHIPS, share, reward_width), BF16), ((16, PATCH), BF16)],
        10**6,
        MIB,
        [embedded, added, post_line, head_line],
        spots,
    )
    slope_half = exchange(slope_copies, ROWS).reshape(half, reward_width)
    gained_embed = (embed_weight.astype(F32) * pre_gain).astype(BF16)
    hidden_embed = mm(gained_embed, up_pair).astype(BF16)
    unit_embed = mt(first_unit.astype(BF16), embed_weight)
    (part_copies,) = kernel_call(
        lambda *refs: back_body(*refs[:-1], reward_width, refs[-1]),
        [((CHIPS, half + 16, PATCH), BF16)],
        3 * 10**8,
        4 * MIB,
        [slope_half, down_pair, hidden, hidden_embed, unit_embed, first_root, reward_lanes],
    )
    parts = exchange(part_copies, ROWS).astype(F32).sum(axis=0)
    direct = lax.optimization_barrier(mt(slope_half, embed_weight))
    direct = jnp.concatenate([direct, jnp.zeros((16, PATCH), F32)], axis=0)
    both = parts + direct
    back = swap(both)
    reward = both + back
    reward = reward[half, 0] + reward[half, 1] + reward[half, 2]
    unit_weight, unit_latent, row_inverse = kernel_call(
        unit_body,
        [((rows, HEAD), F32), ((rows, PATCH), F32), ((rows, 1), F32)],
        6 * 10**8,
        4 * MIB,
        [unit_half, unit_other, own_weight, gained16],
        spots,
    )
    query_slope, noise_slope = kernel_call(
        slope_body,
        [((rows, HEAD), BF16), ((rows, PATCH), BF16)],
        6 * 10**8,
        5 * MIB,
        [
            both,
            back,
            crop[:, None],
            crop[None, :],
            weight_latent,
            mean_line,
            sum_line,
            unit_weight,
            unit_latent,
            row_inverse,
            attended,
            weights,
            denominator,
            mine,
            other,
        ],
        consts,
    )

    (spread,) = kernel_call(
        spread_body,
        [((CHIPS, tokens, 2 * HEAD), BF16)],
        10**8,
        MIB,
        [query_slope, swap(query_slope), label],
        core_scalar,
        limit=16 * MIB,
    )
    home = exchange(spread, CHIP)
    (grad_queries,) = kernel_call(
        home_body, [((tokens, HEADS * HEAD), BF16)], 10**6, MIB, [home], limit=16 * MIB
    )
    (grad_stream,) = kernel_call(
        stream_body,
        [((tokens, width), BF16)],
        6 * 10**8,
        5 * MIB,
        [unit_half, unit_other, label, noise_slope, final_weight, gain_line],
        spots,
    )
    return (jnp.reshape(reward, (1,)), grad_stream[None], grad_queries[None])


DP = ("x", "zl")
CTX = ("zh", "y", "core")


def solution(mesh):
    across = mesh.shape["dp"]
    near = min(4, across)
    fine = Mesh(
        mesh.devices.reshape(across // near, near, 2, 4, 2), ("x", "zl", "zh", "y", "core")
    )
    return jax.shard_map(
        step,
        mesh=fine,
        in_specs=(
            P(DP, CTX, None),
            P(DP, CTX, None),
            P(DP, CTX, None),
            P(DP, CTX, None),
            P(DP),
            P(DP, None),
            P(DP, None),
            P(CTX, DP),
            P(),
            P(DP, CTX, None),
            P(DP),
            P(DP, None),
            P(),
            P(),
            P(None, CTX),
            P(CTX, None),
            P(),
            P(),
        ),
        out_specs=(P(DP), P(DP, CTX, None), P(DP, CTX, None)),
        check_vma=False,
    )
```
